16 devices in a mesh: rep: 2 (over y, z), data: 8 (over x, core).
Axes of the slice: x: 4, y: 2, z: 1, core: 2. Of those that a mesh axis runs over, the one named last changes fastest.
The devices are a block of a 4x4x8 slice.
Arguments:
- x: bfloat16 [1024, 1536], P(('rep', 'data')), parts along dimension 0
- adapter_id: int32 [1024], P(('rep', 'data')), parts along dimension 0
- w_gate: bfloat16 [1536, 8960], replicated
- w_up: bfloat16 [1536, 8960], replicated
- w_down: bfloat16 [8960, 1536], replicated
- a_gate: bfloat16 [1024, 8, 1536], P('data')
- b_gate: bfloat16 [1024, 8, 8960], P('data')
- a_up: bfloat16 [1024, 8, 1536], P('data')
- b_up: bfloat16 [1024, 8, 8960], P('data')
- a_down: bfloat16 [1024, 8, 8960], P('data')
- b_down: bfloat16 [1024, 8, 1536], P('data')
Outputs:
- output: bfloat16 [1024, 1536], P(('rep', 'data')), parts along dimension 0
There are 2 independent parts. The reference program is written for one: setup_inputs(seed, part) draws one part's arguments, and reference() takes and returns one part's arrays. A program takes and returns all parts, laid end to end along the dimension named above; an argument that names none is the same for every part.
All inputs are finite; a program needn't handle non-finite values.
Results may differ from the reference program's by a relative error of at most 0.00571002.
Values are sent between devices in bfloat16 or wider.
A program may use at most 768 MiB of HBM per device.

```python
import jax
import jax.numpy as jnp
from jax import lax

D = 1536
FF = 8960
RANK = 8
ADAPTERS = 1024
TOK = 64
GROUP = 8
CAP = 24
LORA_ALPHA = 32

SCALE = LORA_ALPHA / RANK
TOKENS = TOK * GROUP
PER_OWNER = ADAPTERS // GROUP


def shuffle_row(row_key, row_owner):
    return row_owner[jax.random.permutation(row_key, TOK)]


def draw_ids(id_key):
    id_keys = jax.random.split(id_key, 5)
    hot_owner = jax.random.randint(id_keys[0], (), 0, GROUP)
    offset = jax.random.randint(id_keys[1], (), 0, GROUP - 1)
    source = jnp.arange(GROUP)[:, None]
    position = jnp.arange(TOK)[None, :]
    spread = (offset + source * (TOK - CAP) + position - CAP) % (GROUP - 1)
    owner_idx = jnp.where(position < CAP, hot_owner, (hot_owner + 1 + spread) % GROUP)
    owner_idx = jax.vmap(shuffle_row)(jax.random.split(id_keys[2], GROUP), owner_idx)
    flat_owner = owner_idx.reshape(TOKENS)
    owner_hot = (flat_owner[:, None] == jnp.arange(GROUP)[None, :]).astype(jnp.int32)
    arrival = jnp.sum(jnp.cumsum(owner_hot, axis=0) * owner_hot, axis=1) - 1
    popular = jnp.minimum(jax.random.randint(id_keys[3], (TOKENS,), 0, PER_OWNER), jax.random.randint(id_keys[4], (TOKENS,), 0, PER_OWNER))
    local_idx = jnp.where(arrival == 0, 0, jnp.where(arrival == 1, PER_OWNER - 1, popular))
    return (flat_owner * PER_OWNER + local_idx).astype(jnp.int32)


def setup_inputs(seed: int = 0, part: int = 0) -> dict:
    key = jax.random.key(seed)
    weight_keys = jax.random.split(key, 9)
    part_keys = jax.random.split(jax.random.fold_in(key, part), 2)
    b_scale = 0.3 / (SCALE * RANK ** 0.5)

    def draw_normal(index, shape, std):
        return (jax.random.normal(weight_keys[index], shape, jnp.float32) * std).astype(jnp.bfloat16)

    return {
        "x": jax.random.normal(part_keys[0], (TOKENS, D), jnp.float32).astype(jnp.bfloat16),
        "adapter_id": draw_ids(part_keys[1]),
        "w_gate": draw_normal(0, (D, FF), D ** -0.5),
        "w_up": draw_normal(1, (D, FF), D ** -0.5),
        "w_down": draw_normal(2, (FF, D), FF ** -0.5),
        "a_gate": draw_normal(3, (ADAPTERS, RANK, D), D ** -0.5),
        "b_gate": draw_normal(4, (ADAPTERS, RANK, FF), b_scale),
        "a_up": draw_normal(5, (ADAPTERS, RANK, D), D ** -0.5),
        "b_up": draw_normal(6, (ADAPTERS, RANK, FF), b_scale),
        "a_down": draw_normal(7, (ADAPTERS, RANK, FF), FF ** -0.5),
        "b_down": draw_normal(8, (ADAPTERS, RANK, D), b_scale),
    }


def lora_delta(tok_rows, tok_ids, a_mat, b_mat):
    a_rows = a_mat[tok_ids].astype(jnp.float32)
    b_rows = b_mat[tok_ids].astype(jnp.float32)
    low_rank = jnp.einsum("td,trd->tr", tok_rows.astype(jnp.float32), a_rows).astype(jnp.bfloat16)
    full_rows = jnp.einsum("tr,trf->tf", low_rank.astype(jnp.float32), b_rows)
    return (SCALE * full_rows).astype(jnp.bfloat16)


def reference(x, adapter_id, w_gate, w_up, w_down, a_gate, b_gate, a_up, b_up, a_down, b_down):
    def one_block(block_in):
        tok_rows, tok_ids = block_in
        gate_pre = jnp.dot(tok_rows, w_gate, preferred_element_type=jnp.float32) + lora_delta(tok_rows, tok_ids, a_gate, b_gate).astype(jnp.float32)
        up_pre = jnp.dot(tok_rows, w_up, preferred_element_type=jnp.float32) + lora_delta(tok_rows, tok_ids, a_up, b_up).astype(jnp.float32)
        hidden = (jax.nn.silu(gate_pre) * up_pre).astype(jnp.bfloat16)
        down_out = jnp.dot(hidden, w_down, preferred_element_type=jnp.float32) + lora_delta(hidden, tok_ids, a_down, b_down).astype(jnp.float32)
        return (tok_rows.astype(jnp.float32) + down_out).astype(jnp.bfloat16)

    blocks = (x.reshape(GROUP, TOK, D), adapter_id.reshape(GROUP, TOK))
    return lax.map(one_block, blocks).reshape(TOKENS, D)
```

```python
import jax
import jax.numpy as jnp
from jax import lax
from jax.sharding import PartitionSpec as P

ALPHA = 32


def solution(mesh):
    groups = mesh.shape["data"]
    row_spec = P(("rep", "data"), None)
    id_spec = P(("rep", "data"))
    owned_spec = P("data", None, None)

    def device_step(x, adapter_id, w_gate, w_up, w_down, a_gate, b_gate, a_up, b_up, a_down, b_down):
        tok_count = x.shape[0]
        per_owner, rank, _ = a_gate.shape
        scale = ALPHA / rank
        capacity = (3 * tok_count + groups - 1) // groups
        owner_idx = adapter_id // per_owner
        local_ad = adapter_id % per_owner
        same = (owner_idx[:, None] == owner_idx[None, :]) & (jnp.arange(tok_count)[None, :] < jnp.arange(tok_count)[:, None])
        arrival = jnp.sum(same.astype(jnp.int32), axis=1)
        slot_idx = owner_idx * capacity + arrival
        dispatch = (slot_idx[:, None] == jnp.arange(groups * capacity)[None, :]).astype(jnp.bfloat16)
        id_cols = jnp.broadcast_to(local_ad.astype(jnp.bfloat16)[:, None], (tok_count, 128))
        payload = jnp.concatenate([x, id_cols], axis=1)
        send = jnp.einsum("tm,td->md", dispatch, payload, preferred_element_type=jnp.float32).astype(jnp.bfloat16)
        recv = lax.all_to_all(send, "data", 0, 0, tiled=True)
        rows = recv[:, : x.shape[1]]
        ids = recv[:, x.shape[1] : x.shape[1] + 1].astype(jnp.int32)
        own = ids == (jnp.arange(per_owner * rank) // rank)[None, :]

        def delta(v, a_mat, b_mat):
            low = lax.dot_general(v, a_mat.reshape(per_owner * rank, -1), (((1,), (1,)), ((), ())), preferred_element_type=jnp.float32)
            low = jnp.where(own, low, 0.0).astype(jnp.bfloat16)
            full = jnp.dot(low, b_mat.reshape(per_owner * rank, -1), preferred_element_type=jnp.float32)
            return (scale * full).astype(jnp.bfloat16).astype(jnp.float32)

        gate_pre = jnp.dot(rows, w_gate, preferred_element_type=jnp.float32) + delta(rows, a_gate, b_gate)
        up_pre = jnp.dot(rows, w_up, preferred_element_type=jnp.float32) + delta(rows, a_up, b_up)
        hidden = (jax.nn.silu(gate_pre) * up_pre).astype(jnp.bfloat16)
        down = jnp.dot(hidden, w_down, preferred_element_type=jnp.float32) + delta(hidden, a_down, b_down)
        done = (rows.astype(jnp.float32) + down).astype(jnp.bfloat16)
        back = lax.all_to_all(done, "data", 0, 0, tiled=True)
        return jnp.einsum("tm,md->td", dispatch, back, preferred_element_type=jnp.float32).astype(jnp.bfloat16)

    return jax.shard_map(device_step, mesh=mesh, in_specs=(row_spec, id_spec, P(), P(), P(), owned_spec, owned_spec, owned_spec, owned_spec, owned_spec, owned_spec), out_specs=row_spec, check_vma=False)
```

```python
import functools

import jax
import jax.numpy as jnp
from jax import lax
from jax.experimental import pallas as pl
from jax.experimental.pallas import tpu as pltpu
from jax.sharding import PartitionSpec as P

ALPHA = 32
ID_LANES = 128
SUB = 256
STEP_SUBS = 5
BF = jnp.bfloat16
F32 = jnp.float32


def nn(a, b):
    return jnp.dot(a, b, preferred_element_type=F32)


def nt(a, b):
    return lax.dot_general(a, b, (((1,), (1,)), ((), ())), preferred_element_type=F32)


def count_ge(v, width, groups):
    total = jnp.zeros(v.shape, jnp.int32)
    for g in range(1, groups):
        total += (v >= g * width).astype(jnp.int32)
    return total


def layer_kernel(groups, rank, cap, per_owner, x_ref, ids_ref, wg, wu, wd, ag, au, bg, bu, ad, bd, out_ref,
                 send, recv, rows, low_g, low_u, hid, low_d, ret, got, a_buf, b_buf, big,
                 ring_sem, a_sem, b_sem, wd_sem, out_sem, in_sem, rs_sem, rr_sem):
    toks, width = x_ref.shape
    ff = wg.shape[1]
    ranks = per_owner * rank
    slots = groups * cap
    scale = ALPHA / rank
    step = STEP_SUBS * SUB
    n_steps = ff // step
    ring_rows = 2 * width + 3 * ranks
    fold = ff // STEP_SUBS
    cols = width // SUB
    parts = ((wg, 0, width), (wu, width, width), (bg, 2 * width, ranks), (bu, 2 * width + ranks, ranks), (ad, 2 * width + 2 * ranks, ranks))
    me = lax.axis_index("data")
    peers = [lax.rem(me + k, groups) for k in (4, 3, 5, 2, 6, 1, 7) if k < groups]

    def ring_copy(c, i):
        src, off, n = parts[i]
        slot = lax.rem(c, 2)
        start = pl.multiple_of(slot * ring_rows + off, 8)
        col = pl.multiple_of(c * step, 128)
        return pltpu.make_async_copy(src.at[:, pl.ds(col, step)], big.at[pl.ds(start, n), :], ring_sem.at[slot, i])

    def wd_at(j):
        return pl.multiple_of(2 * ring_rows + (1 - j) * fold, 8)

    def wd_copy(j, q):
        col = pl.multiple_of(j * SUB, 128)
        return pltpu.make_async_copy(wd.at[pl.ds(q * fold, fold), pl.ds(col, SUB)], big.at[pl.ds(wd_at(j), fold), pl.ds(q * SUB, SUB)], wd_sem.at[j, q])

    def start_wd(j):
        for q in range(STEP_SUBS):
            wd_copy(j, q).start()

    a_copies = [pltpu.make_async_copy(src, a_buf.at[i], a_sem.at[i]) for i, src in enumerate((ag, au))]
    b_copy = pltpu.make_async_copy(bd, b_buf, b_sem)
    for cp in a_copies:
        cp.start()
    for c in range(2):
        for i in range(len(parts)):
            ring_copy(c, i).start()

    barrier = pltpu.get_barrier_semaphore()
    for p in peers:
        pl.semaphore_signal(barrier, inc=1, device_id={"data": p}, device_id_type=pl.DeviceIdType.MESH)

    id_row = ids_ref[...]
    sub_i = lax.broadcasted_iota(jnp.int32, (toks, toks), 0)
    lane_i = lax.broadcasted_iota(jnp.int32, (toks, toks), 1)
    id_col = jnp.sum(jnp.where(sub_i == lane_i, jnp.broadcast_to(id_row, (toks, toks)), 0), axis=1, keepdims=True)
    own_row = count_ge(id_row, per_owner, groups)
    own_col = count_ge(id_col, per_owner, groups)
    same = own_col == own_row
    arr_col = jnp.sum((same & (lane_i < sub_i)).astype(jnp.int32), axis=1, keepdims=True)
    arr_row = jnp.sum((same & (sub_i < lane_i)).astype(jnp.int32), axis=0, keepdims=True)
    to_slot = (lax.broadcasted_iota(jnp.int32, (slots, toks), 0) == own_row * cap + arr_row).astype(F32).astype(BF)
    local = (id_col - own_col * per_owner).astype(F32).astype(BF)
    payload = jnp.concatenate([x_ref[...], jnp.broadcast_to(local, (toks, ID_LANES))], axis=1)
    send[...] = nn(to_slot, payload).reshape(groups, cap, width + ID_LANES).astype(BF)

    pl.semaphore_wait(barrier, groups - 1)

    def row_copy(p):
        return pltpu.make_async_remote_copy(src_ref=send.at[p], dst_ref=recv.at[me], send_sem=out_sem.at[p], recv_sem=in_sem.at[me],
                                            device_id={"data": p}, device_id_type=pl.DeviceIdType.MESH)

    def row_arrival(p):
        return pltpu.make_async_remote_copy(src_ref=send.at[p], dst_ref=recv.at[p], send_sem=out_sem.at[p], recv_sem=in_sem.at[p],
                                            device_id={"data": p}, device_id_type=pl.DeviceIdType.MESH)

    for p in peers:
        row_copy(p).start()
    recv[me] = send[me]
    for p in peers:
        row_arrival(p).wait_recv()

    b_copy.start()
    start_wd(0)
    start_wd(1)

    landed = recv[...].astype(F32).reshape(slots, width + ID_LANES)
    rows[...] = landed[:, :width].astype(BF)
    first = landed[:, width:width + 1].astype(jnp.int32) * rank
    rank_i = lax.broadcasted_iota(jnp.int32, (slots, ranks), 1)
    own = (rank_i >= first) & (rank_i < first + rank)
    for i, low in enumerate((low_g, low_u)):
        a_copies[i].wait()
        low[...] = jnp.where(own, nt(rows[...], a_buf[i]), 0.0).astype(BF)
    low_d[...] = jnp.zeros_like(low_d)

    def half(base, col, w_off, w_n, b_off, low):
        full = nn(low[...], big[pl.ds(base + b_off, ranks), col])
        return nn(rows[...], big[pl.ds(base + w_off, w_n), col]) + (scale * full).astype(BF).astype(F32)

    def ff_step(c, carry):
        for i in range(len(parts)):
            ring_copy(c, i).wait()
        base = pl.multiple_of(lax.rem(c, 2) * ring_rows, 8)
        for s in range(STEP_SUBS):
            col = pl.ds(s * SUB, SUB)
            g = half(base, col, 0, width, 2 * width, low_g)
            u = half(base, col, width, width, 2 * width + ranks, low_u)
            hid[c * STEP_SUBS + s] = (g * jax.nn.sigmoid(g) * u).astype(BF)
        h = jnp.concatenate([hid[c * STEP_SUBS + s] for s in range(STEP_SUBS)], axis=1)
        low_d[...] += nt(h, big[pl.ds(base + 2 * width + 2 * ranks, ranks), :])

        @pl.when(c + 2 < n_steps)
        def _():
            for i in range(len(parts)):
                ring_copy(c + 2, i).start()

        @pl.when(c == n_steps - 2)
        def _():
            for j in range(2, 5):
                start_wd(j)

        return carry

    lax.fori_loop(0, n_steps, ff_step, 0)
    start_wd(5)

    low_dm = jnp.where(own, low_d[...], 0.0).astype(BF)
    low_g[...] = low_dm
    b_copy.wait()

    def back_copy(j, p):
        return pltpu.make_async_remote_copy(src_ref=ret.at[j, p], dst_ref=got.at[j, me], send_sem=rs_sem.at[j, p], recv_sem=rr_sem.at[j, me],
                                            device_id={"data": p}, device_id_type=pl.DeviceIdType.MESH)

    def back_arrival(j, p):
        return pltpu.make_async_remote_copy(src_ref=ret.at[j, p], dst_ref=got.at[j, p], send_sem=rs_sem.at[j, p], recv_sem=rr_sem.at[j, p],
                                            device_id={"data": p}, device_id_type=pl.DeviceIdType.MESH)

    def col_step(j, carry):
        for q in range(STEP_SUBS):
            wd_copy(j, q).wait()
        col = pl.ds(pl.multiple_of(j * SUB, 128), SUB)
        full = nn(low_g[...], b_buf[:, col])
        per = fold // SUB
        acc = jnp.zeros((slots, SUB), F32)
        for q in range(STEP_SUBS):
            h = jnp.concatenate([hid[q * per + s] for s in range(per)], axis=1)
            acc += nn(h, big[pl.ds(wd_at(j), fold), pl.ds(q * SUB, SUB)])
        done = rows[:, col].astype(F32) + (acc + (scale * full).astype(BF).astype(F32))
        ret[j] = done.reshape(groups, cap, SUB).astype(BF)
        for p in peers:
            back_copy(j, p).start()
        got[j, me] = ret[j, me]
        return carry

    lax.fori_loop(0, cols, col_step, 0)

    to_tok = (lax.broadcasted_iota(jnp.int32, (toks, slots), 1) == own_col * cap + arr_col).astype(F32).astype(BF)
    for j in range(cols):
        for p in peers:
            back_arrival(j, p).wait_recv()
        block = got[j].astype(F32).reshape(slots, SUB).astype(BF)
        out_ref[:, j * SUB:(j + 1) * SUB] = nn(to_tok, block).astype(BF)
    for p in peers:
        row_copy(p).wait_send()
        for j in range(cols):
            back_copy(j, p).wait_send()


def solution(mesh):
    groups = mesh.shape["data"]
    row_spec = P(("rep", "data"), None)
    id_spec = P(("rep", "data"))
    owned_spec = P("data", None, None)

    def device_step(x, adapter_id, w_gate, w_up, w_down, a_gate, b_gate, a_up, b_up, a_down, b_down):
        toks, width = x.shape
        per_owner, rank, ff = b_gate.shape
        ranks = per_owner * rank
        cap = (3 * toks + groups - 1) // groups
        slots = groups * cap
        cols = width // SUB
        ring_rows = 2 * width + 3 * ranks
        fold = ff // STEP_SUBS

        def flat(m):
            return m.reshape(ranks, m.shape[-1])

        return pl.pallas_call(
            functools.partial(layer_kernel, groups, rank, cap, per_owner),
            out_shape=jax.ShapeDtypeStruct((toks, width), BF),
            in_specs=[pl.BlockSpec(memory_space=pltpu.VMEM)] * 2 + [pl.BlockSpec(memory_space=pl.ANY)] * 9,
            out_specs=pl.BlockSpec(memory_space=pltpu.VMEM),
            scratch_shapes=[
                pltpu.VMEM((groups, cap, width + ID_LANES), BF),
                pltpu.VMEM((groups, cap, width + ID_LANES), BF),
                pltpu.VMEM((slots, width), BF),
                pltpu.VMEM((slots, ranks), BF),
                pltpu.VMEM((slots, ranks), BF),
                pltpu.VMEM((ff // SUB, slots, SUB), BF),
                pltpu.VMEM((slots, ranks), F32),
                pltpu.VMEM((cols, groups, cap, SUB), BF),
                pltpu.VMEM((cols, groups, cap, SUB), BF),
                pltpu.VMEM((2, ranks, width), BF),
                pltpu.VMEM((ranks, width), BF),
                pltpu.VMEM((2 * ring_rows + 2 * fold, STEP_SUBS * SUB), BF),
                pltpu.SemaphoreType.DMA((2, 5)),
                pltpu.SemaphoreType.DMA((2,)),
                pltpu.SemaphoreType.DMA,
                pltpu.SemaphoreType.DMA((cols, STEP_SUBS)),
                pltpu.SemaphoreType.DMA((groups,)),
                pltpu.SemaphoreType.DMA((groups,)),
                pltpu.SemaphoreType.DMA((cols, groups)),
                pltpu.SemaphoreType.DMA((cols, groups)),
            ],
            compiler_params=pltpu.CompilerParams(collective_id=0, has_side_effects=True, vmem_limit_bytes=67_000_000),
            name="lora_layer",
        )(x, adapter_id.reshape(1, toks), w_gate, w_up, w_down, flat(a_gate), flat(a_up), flat(b_gate), flat(b_up), flat(a_down), flat(b_down))

    return jax.shard_map(device_step, mesh=mesh, in_specs=(row_spec, id_spec, P(), P(), P(), owned_spec, owned_spec, owned_spec, owned_spec, owned_spec, owned_spec), out_specs=row_spec, check_vma=False)
```

```python
import functools

import jax
import jax.numpy as jnp
from jax import lax
from jax.experimental import pallas as pl
from jax.experimental.pallas import tpu as pltpu
from jax.sharding import PartitionSpec as P

ALPHA = 32
ID_LANES = 128
SUB = 256
STEP_SUBS = 5
RING = 3
BF = jnp.bfloat16
F32 = jnp.float32


def nn(a, b):
    return jnp.dot(a, b, preferred_element_type=F32)


def nt(a, b):
    return lax.dot_general(a, b, (((1,), (1,)), ((), ())), preferred_element_type=F32)


def count_ge(v, width, groups):
    total = jnp.zeros(v.shape, jnp.int32)
    for g in range(1, groups):
        total += (v >= g * width).astype(jnp.int32)
    return total


def layer_kernel(groups, rank, cap, per_owner, x_ref, ids_ref, wg, wu, wd, ag, au, bg, bu, ad, bd, out_ref,
                 send, recv, rows, low_g, low_u, hid, low_d, ret, got, b_buf, big,
                 ring_sem, a_sem, b_sem, wd_sem, out_sem, in_sem, rs_sem, rr_sem):
    toks, width = x_ref.shape
    ff = wg.shape[1]
    ranks = per_owner * rank
    slots = groups * cap
    scale = ALPHA / rank
    step = STEP_SUBS * SUB
    n_steps = ff // step
    ring_rows = 2 * width + 3 * ranks
    fold = ff // STEP_SUBS
    cols = width // SUB
    parts = ((wg, 0, width), (wu, width, width), (bg, 2 * width, ranks), (bu, 2 * width + ranks, ranks), (ad, 2 * width + 2 * ranks, ranks))
    me = lax.axis_index("data")
    peers = [lax.rem(me + k, groups) for k in (4, 3, 5, 2, 6, 1, 7) if k < groups]

    def ring_copy(c, i):
        src, off, n = parts[i]
        slot = lax.rem(c, RING)
        start = pl.multiple_of(slot * ring_rows + off, 8)
        col = pl.multiple_of(c * step, 128)
        return pltpu.make_async_copy(src.at[:, pl.ds(col, step)], big.at[pl.ds(start, n), :], ring_sem.at[slot])

    def landing(dst, sem):
        return pltpu.make_async_copy(dst, dst, sem)

    def ring_wait(c):
        slot = lax.rem(c, RING)
        landing(big.at[pl.ds(pl.multiple_of(slot * ring_rows, 8), ring_rows), :], ring_sem.at[slot]).wait()

    def wd_at(j):
        return pl.multiple_of(ring_rows * (1 + j // 3) + lax.rem(j, 3) * fold, 8)

    def wd_copy(j, q):
        col = pl.multiple_of(j * SUB, 128)
        return pltpu.make_async_copy(wd.at[pl.ds(q * fold, fold), pl.ds(col, SUB)], big.at[pl.ds(wd_at(j), fold), pl.ds(q * SUB, SUB)], wd_sem.at[j])

    def start_wd(j):
        for q in range(STEP_SUBS):
            wd_copy(j, q).start()

    rest = width - step
    a_base = (RING - 1) * ring_rows
    a_copies = []
    for i, src in enumerate((ag, au)):
        a_copies.append(pltpu.make_async_copy(src.at[:, :step], big.at[pl.ds(a_base + i * ranks, ranks), :], a_sem.at[i]))
        a_copies.append(pltpu.make_async_copy(src.at[:, step:], big.at[pl.ds(a_base + 2 * ranks, ranks), pl.ds(i * rest, rest)], a_sem.at[i]))
    b_copy = pltpu.make_async_copy(bd, b_buf, b_sem)
    for cp in a_copies:
        cp.start()
    for c in range(2):
        for i in range(len(parts)):
            ring_copy(c, i).start()
    b_copy.start()

    barrier = pltpu.get_barrier_semaphore()
    for p in peers:
        pl.semaphore_signal(barrier, inc=1, device_id={"data": p}, device_id_type=pl.DeviceIdType.MESH)

    id_row = ids_ref[...]
    sub_i = lax.broadcasted_iota(jnp.int32, (toks, toks), 0)
    lane_i = lax.broadcasted_iota(jnp.int32, (toks, toks), 1)
    id_col = jnp.sum(jnp.where(sub_i == lane_i, jnp.broadcast_to(id_row, (toks, toks)), 0), axis=1, keepdims=True)
    own_row = count_ge(id_row, per_owner, groups)
    own_col = count_ge(id_col, per_owner, groups)
    same = own_col == own_row
    arr_col = jnp.sum((same & (lane_i < sub_i)).astype(jnp.int32), axis=1, keepdims=True)
    arr_row = jnp.sum((same & (sub_i < lane_i)).astype(jnp.int32), axis=0, keepdims=True)
    to_slot = (lax.broadcasted_iota(jnp.int32, (slots, toks), 0) == own_row * cap + arr_row).astype(F32).astype(BF)
    local = (id_col - own_col * per_owner).astype(F32).astype(BF)
    payload = jnp.concatenate([x_ref[...], jnp.broadcast_to(local, (toks, ID_LANES))], axis=1)
    send[...] = nn(to_slot, payload).reshape(groups, cap, width + ID_LANES).astype(BF)

    with jax.named_scope('entry_wait'):
        pl.semaphore_wait(barrier, groups - 1)

    def row_copy(p):
        return pltpu.make_async_remote_copy(src_ref=send.at[p], dst_ref=recv.at[me], send_sem=out_sem, recv_sem=in_sem,
                                            device_id={"data": p}, device_id_type=pl.DeviceIdType.MESH)

    for p in peers:
        row_copy(p).start()
    recv[me] = send[me]
    with jax.named_scope('row_wait'):
        landing(recv.at[:groups - 1], in_sem).wait()

    landed = recv[...].astype(F32).reshape(slots, width + ID_LANES)
    rows[...] = landed[:, :width].astype(BF)
    first = landed[:, width:width + 1].astype(jnp.int32) * rank
    rank_i = lax.broadcasted_iota(jnp.int32, (slots, ranks), 1)
    own = (rank_i >= first) & (rank_i < first + rank)
    for i in range(2):
        landing(b_buf, a_sem.at[i]).wait()
    for i, low in enumerate((low_g, low_u)):
        acc = nt(rows[:, :step], big[a_base + i * ranks:a_base + (i + 1) * ranks, :])
        acc += nt(rows[:, step:], big[a_base + 2 * ranks:a_base + 3 * ranks, i * rest:(i + 1) * rest])
        low[...] = jnp.where(own, acc, 0.0).astype(BF)
    for i in range(len(parts)):
        ring_copy(RING - 1, i).start()
    low_d[...] = jnp.zeros_like(low_d)

    def half(base, col, w_off, w_n, b_off, low):
        full = nn(low[...], big[pl.ds(base + b_off, ranks), col])
        return nn(rows[...], big[pl.ds(base + w_off, w_n), col]) + (scale * full).astype(BF).astype(F32)

    def ff_step(c, carry):
        with jax.named_scope('ring_wait'):
            ring_wait(c)
        base = pl.multiple_of(lax.rem(c, RING) * ring_rows, 8)

        def gate_up(s):
            col = pl.ds(s * SUB, SUB)
            return half(base, col, 0, width, 2 * width, low_g), half(base, col, width, width, 2 * width + ranks, low_u)

        def add_low(lo, hi):
            h = jnp.concatenate([hid[c * STEP_SUBS + s] for s in range(lo, hi)], axis=1)
            low_d[...] += nt(h, big[pl.ds(base + 2 * width + 2 * ranks, ranks), lo * SUB:hi * SUB])

        for s in range(STEP_SUBS):
            g, u = gate_up(s)
            hid[c * STEP_SUBS + s] = (g * jax.nn.sigmoid(g) * u).astype(BF)
        add_low(0, STEP_SUBS)

        @pl.when(c + RING < n_steps)
        def _():
            for i in range(len(parts)):
                ring_copy(c + RING, i).start()

        for back in (0, 1):
            @pl.when(c == n_steps - 3 + back)
            def _(back=back):
                for j in range(3 * back, 3 * back + 3):
                    start_wd(j)

        return carry

    lax.fori_loop(0, n_steps, ff_step, 0)

    low_dm = jnp.where(own, low_d[...], 0.0).astype(BF)
    low_g[...] = low_dm
    b_copy.wait()

    def back_copy(j, p):
        return pltpu.make_async_remote_copy(src_ref=ret.at[j, p], dst_ref=got.at[j, me], send_sem=rs_sem, recv_sem=rr_sem.at[j],
                                            device_id={"data": p}, device_id_type=pl.DeviceIdType.MESH)

    def col_step(j, carry):
        with jax.named_scope('wd_wait'):
            landing(big.at[pl.ds(wd_at(j), fold), :], wd_sem.at[j]).wait()
        col = pl.ds(pl.multiple_of(j * SUB, 128), SUB)
        full = nn(low_g[...], b_buf[:, col])
        h = jnp.concatenate([hid[s] for s in range(ff // SUB)], axis=1)
        w = jnp.concatenate([big[pl.ds(wd_at(j), fold), pl.ds(q * SUB, SUB)] for q in range(STEP_SUBS)], axis=0)
        acc = nn(h, w)
        done = rows[:, col].astype(F32) + (acc + (scale * full).astype(BF).astype(F32))
        ret[j] = done.reshape(groups, cap, SUB).astype(BF)
        for p in peers:
            back_copy(j, p).start()
        got[j, me] = ret[j, me]
        return carry

    lax.fori_loop(0, cols, col_step, 0)

    to_tok = (lax.broadcasted_iota(jnp.int32, (toks, slots), 1) == own_col * cap + arr_col).astype(F32).astype(BF)
    for j in range(cols):
        with jax.named_scope('back_wait'):
            landing(got.at[j, :groups - 1], rr_sem.at[j]).wait()
        block = got[j].astype(F32).reshape(slots, SUB).astype(BF)
        out_ref[:, j * SUB:(j + 1) * SUB] = nn(to_tok, block).astype(BF)
    with jax.named_scope('send_wait'):
        landing(send.at[:groups - 1], out_sem).wait()
        landing(ret.at[:, :groups - 1], rs_sem).wait()


def solution(mesh):
    groups = mesh.shape["data"]
    row_spec = P(("rep", "data"), None)
    id_spec = P(("rep", "data"))
    owned_spec = P("data", None, None)

    def device_step(x, adapter_id, w_gate, w_up, w_down, a_gate, b_gate, a_up, b_up, a_down, b_down):
        toks, width = x.shape
        per_owner, rank, ff = b_gate.shape
        ranks = per_owner * rank
        cap = (3 * toks + groups - 1) // groups
        slots = groups * cap
        cols = width // SUB
        ring_rows = 2 * width + 3 * ranks

        def flat(m):
            return m.reshape(ranks, m.shape[-1])

        return pl.pallas_call(
            functools.partial(layer_kernel, groups, rank, cap, per_owner),
            out_shape=pltpu.VMEM((toks, width), BF),
            in_specs=[pl.BlockSpec(memory_space=pltpu.VMEM)] * 2 + [pl.BlockSpec(memory_space=pl.ANY)] * 9,
            out_specs=pl.BlockSpec(memory_space=pltpu.VMEM),
            scratch_shapes=[
                pltpu.VMEM((groups, cap, width + ID_LANES), BF),
                pltpu.VMEM((groups, cap, width + ID_LANES), BF),
                pltpu.VMEM((slots, width), BF),
                pltpu.VMEM((slots, ranks), BF),
                pltpu.VMEM((slots, ranks), BF),
                pltpu.VMEM((ff // SUB, slots, SUB), BF),
                pltpu.VMEM((slots, ranks), F32),
                pltpu.VMEM((cols, groups, cap, SUB), BF),
                pltpu.VMEM((cols, groups, cap, SUB), BF),
                pltpu.VMEM((ranks, width), BF),
                pltpu.VMEM((RING * ring_rows, STEP_SUBS * SUB), BF),
                pltpu.SemaphoreType.DMA((RING,)),
                pltpu.SemaphoreType.DMA((2,)),
                pltpu.SemaphoreType.DMA,
                pltpu.SemaphoreType.DMA((cols,)),
                pltpu.SemaphoreType.DMA,
                pltpu.SemaphoreType.DMA,
                pltpu.SemaphoreType.DMA,
                pltpu.SemaphoreType.DMA((cols,)),
            ],
            compiler_params=pltpu.CompilerParams(collective_id=0, has_side_effects=True, vmem_limit_bytes=64_000_000),
            name="lora_layer",
        )(x, adapter_id.reshape(1, toks), w_gate, w_up, w_down, flat(a_gate), flat(a_up), flat(b_gate), flat(b_up), flat(a_down), flat(b_down))

    return jax.shard_map(device_step, mesh=mesh, in_specs=(row_spec, id_spec, P(), P(), P(), owned_spec, owned_spec, owned_spec, owned_spec, owned_spec, owned_spec), out_specs=row_spec, check_vma=False)
```

```python
import functools

import jax
import jax.numpy as jnp
from jax import lax
from jax.experimental import pallas as pl
from jax.experimental.pallas import tpu as pltpu
from jax.sharding import PartitionSpec as P

ALPHA = 32
ID_LANES = 128
SUB = 256
STEP_SUBS = 5
RING = 3
PAIRS = 2
BF = jnp.bfloat16
F32 = jnp.float32


def nn(a, b):
    return jnp.dot(a, b, preferred_element_type=F32)


def nt(a, b):
    return lax.dot_general(a, b, (((1,), (1,)), ((), ())), preferred_element_type=F32)


def count_ge(v, width, groups):
    total = jnp.zeros(v.shape, jnp.int32)
    for g in range(1, groups):
        total += (v >= g * width).astype(jnp.int32)
    return total


def layer_kernel(groups, rank, cap, per_owner, x_ref, ids_ref, wg, wu, wd, ag, au, bg, bu, ad, bd, out_ref,
                 send, recv, rows, low_g, low_u, hid, low_d, ret, got, b_buf, ad_t, big,
                 ring_sem, a_sem, b_sem, wd_sem, out_sem, in_sem, rs_sem, rr_sem):
    toks, width = x_ref.shape
    ff = wg.shape[1]
    ranks = per_owner * rank
    slots = groups * cap
    scale = ALPHA / rank
    step = STEP_SUBS * SUB
    n_steps = ff // step
    ring_rows = 2 * width + 3 * ranks
    fold = ff // STEP_SUBS
    cols = width // SUB
    parts = ((wg, 0, width), (wu, width, width), (bg, 2 * width, ranks), (bu, 2 * width + ranks, ranks), (ad, 2 * width + 2 * ranks, ranks))
    me = lax.axis_index("data")
    peers = [lax.rem(me + k, groups) for k in (4, 3, 5, 2, 6, 1, 7) if k < groups]

    def ring_copy(c, i):
        src, off, n = parts[i]
        slot = lax.rem(c, RING)
        start = pl.multiple_of(slot * ring_rows + off, 8)
        col = pl.multiple_of(c * step, 128)
        return pltpu.make_async_copy(src.at[:, pl.ds(col, step)], big.at[pl.ds(start, n), :], ring_sem.at[slot])

    def landing(dst, sem):
        return pltpu.make_async_copy(dst, dst, sem)

    def ring_wait(c):
        slot = lax.rem(c, RING)
        landing(big.at[pl.ds(pl.multiple_of(slot * ring_rows, 8), ring_rows), :], ring_sem.at[slot]).wait()

    def wd_at(j):
        return pl.multiple_of(ring_rows * (1 + j // 3) + lax.rem(j, 3) * fold, 8)

    def wd_copy(j, q):
        col = pl.multiple_of(j * SUB, 128)
        return pltpu.make_async_copy(wd.at[pl.ds(q * fold, fold), pl.ds(col, SUB)], big.at[pl.ds(wd_at(j), fold), pl.ds(q * SUB, SUB)], wd_sem.at[j])

    def start_wd(j):
        for q in range(STEP_SUBS):
            wd_copy(j, q).start()

    rest = width - step
    t_base = (RING - 1) * ring_rows
    a_base = t_base + 2 * width
    a_copies = []
    for i, src in enumerate((ag, au)):
        a_copies.append(pltpu.make_async_copy(src.at[:, :step], big.at[pl.ds(a_base + i * ranks, ranks), :], a_sem.at[i]))
        a_copies.append(pltpu.make_async_copy(src.at[:, step:], big.at[pl.ds(a_base + 2 * ranks, ranks), pl.ds(i * rest, rest)], a_sem.at[i]))
    b_copy = pltpu.make_async_copy(bd, b_buf, b_sem)
    for cp in a_copies:
        cp.start()
    for c in range(2):
        for i in range(len(parts)):
            ring_copy(c, i).start()
    b_copy.start()

    barrier = pltpu.get_barrier_semaphore()
    for p in peers:
        pl.semaphore_signal(barrier, inc=1, device_id={"data": p}, device_id_type=pl.DeviceIdType.MESH)

    id_row = ids_ref[...]
    sub_i = lax.broadcasted_iota(jnp.int32, (toks, toks), 0)
    lane_i = lax.broadcasted_iota(jnp.int32, (toks, toks), 1)
    id_col = jnp.sum(jnp.where(sub_i == lane_i, jnp.broadcast_to(id_row, (toks, toks)), 0), axis=1, keepdims=True)
    own_row = count_ge(id_row, per_owner, groups)
    own_col = count_ge(id_col, per_owner, groups)
    same = own_col == own_row
    arr_col = jnp.sum((same & (lane_i < sub_i)).astype(jnp.int32), axis=1, keepdims=True)
    arr_row = jnp.sum((same & (sub_i < lane_i)).astype(jnp.int32), axis=0, keepdims=True)
    to_slot = (lax.broadcasted_iota(jnp.int32, (slots, toks), 0) == own_row * cap + arr_row).astype(F32).astype(BF)
    local = (id_col - own_col * per_owner).astype(F32).astype(BF)
    payload = jnp.concatenate([x_ref[...], jnp.broadcast_to(local, (toks, ID_LANES))], axis=1)
    send[...] = nn(to_slot, payload).reshape(groups, cap, width + ID_LANES).astype(BF)

    with jax.named_scope('entry_wait'):
        pl.semaphore_wait(barrier, groups - 1)

    def row_copy(p):
        return pltpu.make_async_remote_copy(src_ref=send.at[p], dst_ref=recv.at[me], send_sem=out_sem, recv_sem=in_sem,
                                            device_id={"data": p}, device_id_type=pl.DeviceIdType.MESH)

    for p in peers:
        row_copy(p).start()
    recv[me] = send[me]
    for i in range(2):
        landing(b_buf, a_sem.at[i]).wait()
    for i in range(2):
        for r in range(0, ranks, 128):
            turned = pl.ds(r, 128)
            big[t_base + i * width:t_base + i * width + step, turned] = big[a_base + i * ranks + r:a_base + i * ranks + r + 128, :].T
            big[t_base + i * width + step:t_base + (i + 1) * width, turned] = big[a_base + 2 * ranks + r:a_base + 2 * ranks + r + 128, i * rest:(i + 1) * rest].T
    for i in range(2, len(parts)):
        ring_copy(RING - 1, i).start()
    with jax.named_scope('row_wait'):
        landing(recv.at[:groups - 1], in_sem).wait()

    landed = recv[...].astype(F32).reshape(slots, width + ID_LANES)
    rows[...] = landed[:, :width].astype(BF)
    first = landed[:, width:width + 1].astype(jnp.int32) * rank
    rank_i = lax.broadcasted_iota(jnp.int32, (slots, ranks), 1)
    own = (rank_i >= first) & (rank_i < first + rank)
    lows = [nn(rows[...], big[t_base + i * width:t_base + (i + 1) * width, :ranks]) for i in range(2)]
    low_g[...] = jnp.where(own, lows[0], 0.0).astype(BF)
    low_u[...] = jnp.where(own, lows[1], 0.0).astype(BF)
    for i in range(2):
        ring_copy(RING - 1, i).start()
    low_d[...] = jnp.zeros_like(low_d)

    def half(base, col, w_off, w_n, b_off, low):
        full = nn(low[...], big[pl.ds(base + b_off, ranks), col])
        return nn(rows[...], big[pl.ds(base + w_off, w_n), col]) + (scale * full).astype(BF).astype(F32)

    def ff_step(c, carry):
        with jax.named_scope('ring_wait'):
            ring_wait(c)
        base = pl.multiple_of(lax.rem(c, RING) * ring_rows, 8)

        def gate_up(s):
            col = pl.ds(s * SUB, SUB)
            return half(base, col, 0, width, 2 * width, low_g), half(base, col, width, width, 2 * width + ranks, low_u)

        def add_low(lo, hi):
            h = jnp.concatenate([hid[c * STEP_SUBS + s] for s in range(lo, hi)], axis=1)
            low_d[...] += nn(h, ad_t[lo * SUB:hi * SUB, :])

        for s in range(STEP_SUBS):
            ad_t[s * SUB:(s + 1) * SUB, :] = big[pl.ds(base + 2 * width + 2 * ranks, ranks), s * SUB:(s + 1) * SUB].T
            g, u = gate_up(s)
            hid[c * STEP_SUBS + s] = (g * jax.nn.sigmoid(g) * u).astype(BF)
        add_low(0, STEP_SUBS)

        @pl.when(c + RING < n_steps)
        def _():
            for i in range(len(parts)):
                ring_copy(c + RING, i).start()

        for back in (0, 1):
            @pl.when(c == n_steps - 3 + back)
            def _(back=back):
                for j in range(3 * back, 3 * back + 3):
                    start_wd(j)

        return carry

    lax.fori_loop(0, n_steps, ff_step, 0)

    low_dm = jnp.where(own, low_d[...], 0.0).astype(BF)
    low_g[...] = low_dm
    b_copy.wait()

    def back_copy(j, n, p):
        return pltpu.make_async_remote_copy(src_ref=ret.at[pl.ds(j, n), p], dst_ref=got.at[pl.ds(j, n), me], send_sem=rs_sem, recv_sem=rr_sem.at[j],
                                            device_id={"data": p}, device_id_type=pl.DeviceIdType.MESH)

    def columns(j, n):
        with jax.named_scope('wd_wait'):
            for k in range(n):
                landing(big.at[pl.ds(wd_at(j + k), fold), :], wd_sem.at[j + k]).wait()
        col = pl.ds(pl.multiple_of(j * SUB, 128), n * SUB)
        full = nn(low_g[...], b_buf[:, col])
        h = jnp.concatenate([hid[s] for s in range(ff // SUB)], axis=1)
        w = jnp.concatenate([jnp.concatenate([big[pl.ds(wd_at(j + k), fold), pl.ds(q * SUB, SUB)] for q in range(STEP_SUBS)], axis=0) for k in range(n)], axis=1)
        done = rows[:, col].astype(F32) + (nn(h, w) + (scale * full).astype(BF).astype(F32))
        for k in range(n):
            ret[j + k] = done[:, k * SUB:(k + 1) * SUB].reshape(groups, cap, SUB).astype(BF)
        for p in peers:
            back_copy(j, n, p).start()
        for k in range(n):
            got[j + k, me] = ret[j + k, me]

    def pair_step(i, carry):
        columns(2 * i, 2)
        return carry

    def single_step(j, carry):
        columns(j, 1)
        return carry

    lax.fori_loop(0, PAIRS, pair_step, 0)
    lax.fori_loop(2 * PAIRS, cols, single_step, 0)

    to_tok = (lax.broadcasted_iota(jnp.int32, (toks, slots), 1) == own_col * cap + arr_col).astype(F32).astype(BF)
    for j, n in [(2 * i, 2) for i in range(PAIRS)] + [(j, 1) for j in range(2 * PAIRS, cols)]:
        with jax.named_scope('back_wait'):
            landing(got.at[pl.ds(j, n), :groups - 1], rr_sem.at[j]).wait()
        for k in range(j, j + n):
            block = got[k].astype(F32).reshape(slots, SUB).astype(BF)
            out_ref[:, k * SUB:(k + 1) * SUB] = nn(to_tok, block).astype(BF)
    with jax.named_scope('send_wait'):
        landing(send.at[:groups - 1], out_sem).wait()
        landing(ret.at[:, :groups - 1], rs_sem).wait()


def solution(mesh):
    groups = mesh.shape["data"]
    row_spec = P(("rep", "data"), None)
    id_spec = P(("rep", "data"))
    owned_spec = P("data", None, None)

    def device_step(x, adapter_id, w_gate, w_up, w_down, a_gate, b_gate, a_up, b_up, a_down, b_down):
        toks, width = x.shape
        per_owner, rank, ff = b_gate.shape
        ranks = per_owner * rank
        cap = (3 * toks + groups - 1) // groups
        slots = groups * cap
        cols = width // SUB
        ring_rows = 2 * width + 3 * ranks

        def flat(m):
            return m.reshape(ranks, m.shape[-1])

        return pl.pallas_call(
            functools.partial(layer_kernel, groups, rank, cap, per_owner),
            out_shape=pltpu.VMEM((toks, width), BF),
            in_specs=[pl.BlockSpec(memory_space=pltpu.VMEM)] * 2 + [pl.BlockSpec(memory_space=pl.ANY)] * 9,
            out_specs=pl.BlockSpec(memory_space=pltpu.VMEM),
            scratch_shapes=[
                pltpu.VMEM((groups, cap, width + ID_LANES), BF),
                pltpu.VMEM((groups, cap, width + ID_LANES), BF),
                pltpu.VMEM((slots, width), BF),
                pltpu.VMEM((slots, ranks), BF),
                pltpu.VMEM((slots, ranks), BF),
                pltpu.VMEM((ff // SUB, slots, SUB), BF),
                pltpu.VMEM((slots, ranks), F32),
                pltpu.VMEM((cols, groups, cap, SUB), BF),
                pltpu.VMEM((cols, groups, cap, SUB), BF),
                pltpu.VMEM((ranks, width), BF),
                pltpu.VMEM((STEP_SUBS * SUB, ranks), BF),
                pltpu.VMEM((RING * ring_rows, STEP_SUBS * SUB), BF),
                pltpu.SemaphoreType.DMA((RING,)),
                pltpu.SemaphoreType.DMA((2,)),
                pltpu.SemaphoreType.DMA,
                pltpu.SemaphoreType.DMA((cols,)),
                pltpu.SemaphoreType.DMA,
                pltpu.SemaphoreType.DMA,
                pltpu.SemaphoreType.DMA,
                pltpu.SemaphoreType.DMA((cols,)),
            ],
            compiler_params=pltpu.CompilerParams(collective_id=0, has_side_effects=True, vmem_limit_bytes=66_400_000),
            name="lora_layer",
        )(x, adapter_id.reshape(1, toks), w_gate, w_up, w_down, flat(a_gate), flat(a_up), flat(b_gate), flat(b_up), flat(a_down), flat(b_down))

    return jax.shard_map(device_step, mesh=mesh, in_specs=(row_spec, id_spec, P(), P(), P(), owned_spec, owned_spec, owned_spec, owned_spec, owned_spec, owned_spec), out_specs=row_spec, check_vma=False)
```

```python
import functools

import jax
import jax.numpy as jnp
from jax import lax
from jax.experimental import pallas as pl
from jax.experimental.pallas import tpu as pltpu
from jax.sharding import PartitionSpec as P

ALPHA = 32
SUB = 256
STEP_SUBS = 5
RING = 3
GROUPS = ((0, 4), (4, 1))
PAIRS = 2
BF = jnp.bfloat16
F32 = jnp.float32


def nn(a, b):
    return jnp.dot(a, b, preferred_element_type=F32)


def nt(a, b):
    return lax.dot_general(a, b, (((1,), (1,)), ((), ())), preferred_element_type=F32)


def count_ge(v, width, groups):
    total = jnp.zeros(v.shape, jnp.int32)
    for g in range(1, groups):
        total += (v >= g * width).astype(jnp.int32)
    return total


def layer_kernel(groups, rank, cap, per_owner, x_ref, ids_ref, wg, wu, wd, ag, au, bg, bu, ad, bd, out_ref,
                 send, recv, rows, low_g, low_u, hid, low_d, ret, got, b_buf, ad_t, big, all_ids, first,
                 ring_sem, a_sem, b_sem, wd_sem, out_sem, in_sem, rs_sem, rr_sem, id_out, id_in):
    toks, width = x_ref.shape
    ff = wg.shape[1]
    ranks = per_owner * rank
    slots = groups * cap
    scale = ALPHA / rank
    step = STEP_SUBS * SUB
    n_steps = ff // step
    ring_rows = 2 * width + 3 * ranks
    fold = ff // STEP_SUBS
    cols = width // SUB
    whole = ((wg, 0, width), (wu, width, width), (bg, 2 * width, ranks), (bu, 2 * width + ranks, ranks), (ad, 2 * width + 2 * ranks, ranks))
    me = lax.axis_index("data")
    peers = [lax.rem(me + k, groups) for k in (4, 3, 5, 2, 6, 1, 7) if k < groups]

    def ring_copy(c, g, i):
        src, off, n = whole[i]
        lo, subs = GROUPS[g]
        slot = lax.rem(c, RING)
        start = pl.multiple_of(slot * ring_rows + off, 8)
        col = pl.multiple_of(c * step + lo * SUB, 128)
        return pltpu.make_async_copy(src.at[:, pl.ds(col, subs * SUB)], big.at[pl.ds(start, n), pl.ds(lo * SUB, subs * SUB)], ring_sem.at[slot, g])

    def start_ring(c, which):
        for g in range(len(GROUPS)):
            for i in which:
                ring_copy(c, g, i).start()

    def landing(dst, sem):
        return pltpu.make_async_copy(dst, dst, sem)

    def ring_wait(c, g):
        slot = lax.rem(c, RING)
        lo, subs = GROUPS[g]
        landing(big.at[pl.ds(pl.multiple_of(slot * ring_rows, 8), ring_rows), pl.ds(lo * SUB, subs * SUB)], ring_sem.at[slot, g]).wait()

    def wd_at(j):
        return pl.multiple_of(ring_rows * (1 + j // 3) + lax.rem(j, 3) * fold, 8)

    def wd_copy(j, q):
        col = pl.multiple_of(j * SUB, 128)
        return pltpu.make_async_copy(wd.at[pl.ds(q * fold, fold), pl.ds(col, SUB)], big.at[pl.ds(wd_at(j), fold), pl.ds(q * SUB, SUB)], wd_sem.at[j])

    def start_wd(j):
        for q in range(STEP_SUBS):
            wd_copy(j, q).start()

    rest = width - step
    t_base = (RING - 1) * ring_rows
    a_base = t_base + 2 * width
    a_copies = []
    for i, src in enumerate((ag, au)):
        a_copies.append(pltpu.make_async_copy(src.at[:, :step], big.at[pl.ds(a_base + i * ranks, ranks), :], a_sem.at[i]))
        a_copies.append(pltpu.make_async_copy(src.at[:, step:], big.at[pl.ds(a_base + 2 * ranks, ranks), pl.ds(i * rest, rest)], a_sem.at[i]))
    b_copy = pltpu.make_async_copy(bd, b_buf, b_sem)
    for cp in a_copies:
        cp.start()
    for c in range(2):
        start_ring(c, range(len(whole)))
    b_copy.start()

    barrier = pltpu.get_barrier_semaphore()
    for p in peers:
        pl.semaphore_signal(barrier, inc=1, device_id={"data": p}, device_id_type=pl.DeviceIdType.MESH)

    id_row = ids_ref[...]
    sub_i = lax.broadcasted_iota(jnp.int32, (toks, toks), 0)
    lane_i = lax.broadcasted_iota(jnp.int32, (toks, toks), 1)
    id_col = jnp.sum(jnp.where(sub_i == lane_i, jnp.broadcast_to(id_row, (toks, toks)), 0), axis=1, keepdims=True)
    own_row = count_ge(id_row, per_owner, groups)
    own_col = count_ge(id_col, per_owner, groups)
    same = own_col == own_row
    arr_col = jnp.sum((same & (lane_i < sub_i)).astype(jnp.int32), axis=1, keepdims=True)
    arr_row = jnp.sum((same & (sub_i < lane_i)).astype(jnp.int32), axis=0, keepdims=True)
    to_slot = (lax.broadcasted_iota(jnp.int32, (slots, toks), 0) == own_row * cap + arr_row).astype(F32).astype(BF)
    send[...] = nn(to_slot, x_ref[...]).reshape(groups, cap, width).astype(BF)

    with jax.named_scope('entry_wait'):
        pl.semaphore_wait(barrier, groups - 1)

    def row_copy(p):
        return pltpu.make_async_remote_copy(src_ref=send.at[p], dst_ref=recv.at[me], send_sem=out_sem, recv_sem=in_sem,
                                            device_id={"data": p}, device_id_type=pl.DeviceIdType.MESH)

    def id_copy(p, at):
        return pltpu.make_async_remote_copy(src_ref=ids_ref, dst_ref=all_ids.at[at], send_sem=id_out, recv_sem=id_in.at[at],
                                            device_id={"data": p}, device_id_type=pl.DeviceIdType.MESH)

    for p in peers:
        id_copy(p, me).start()
    for p in peers:
        row_copy(p).start()
    all_ids[me] = ids_ref[...]
    recv[me] = send[me]
    for i in range(2):
        landing(b_buf, a_sem.at[i]).wait()
    for i in range(2):
        for r in range(0, ranks, 128):
            turned = pl.ds(r, 128)
            big[t_base + i * width:t_base + i * width + step, turned] = big[a_base + i * ranks + r:a_base + i * ranks + r + 128, :].T
            big[t_base + i * width + step:t_base + (i + 1) * width, turned] = big[a_base + 2 * ranks + r:a_base + 2 * ranks + r + 128, i * rest:(i + 1) * rest].T
    start_ring(RING - 1, range(2, len(whole)))
    for p in peers:
        id_copy(p, p).wait_recv()
    every = jnp.concatenate([all_ids[g] for g in range(groups)], axis=0)
    every = every - me * per_owner
    mine = ((every >= 0) & (every < per_owner)).astype(F32)
    before = nn(mine.astype(BF), (sub_i < lane_i).astype(F32).astype(BF))
    slot_i = lax.broadcasted_iota(jnp.int32, (cap, toks), 0).astype(F32)
    value = mine * (every * rank).astype(F32)
    first[...] = jnp.concatenate([jnp.sum(jnp.where(slot_i == before[g:g + 1, :], value[g:g + 1, :], 0.0), axis=1, keepdims=True) for g in range(groups)], axis=0).astype(jnp.int32)

    def own():
        rank_i = lax.broadcasted_iota(jnp.int32, (slots, ranks), 1)
        return (rank_i >= first[...]) & (rank_i < first[...] + rank)

    with jax.named_scope('row_wait'):
        landing(recv.at[:groups - 1], in_sem).wait()

    rows[...] = recv[...].astype(F32).reshape(slots, width).astype(BF)
    lows = [nn(rows[...], big[t_base + i * width:t_base + (i + 1) * width, :ranks]) for i in range(2)]
    low_g[...] = jnp.where(own(), lows[0], 0.0).astype(BF)
    low_u[...] = jnp.where(own(), lows[1], 0.0).astype(BF)
    start_ring(RING - 1, range(2))
    low_d[...] = jnp.zeros_like(low_d)

    def half(base, col, w_off, w_n, b_off, low):
        full = nn(low[...], big[pl.ds(base + b_off, ranks), col])
        return nn(rows[...], big[pl.ds(base + w_off, w_n), col]) + (scale * full).astype(BF).astype(F32)

    def ff_step(c, carry):
        base = pl.multiple_of(lax.rem(c, RING) * ring_rows, 8)
        for n, (lo, subs) in enumerate(GROUPS):
            with jax.named_scope('ring_wait'):
                ring_wait(c, n)
            for s in range(lo, lo + subs):
                col = pl.ds(s * SUB, SUB)
                ad_t[s * SUB:(s + 1) * SUB, :] = big[pl.ds(base + 2 * width + 2 * ranks, ranks), col].T
                g = half(base, col, 0, width, 2 * width, low_g)
                u = half(base, col, width, width, 2 * width + ranks, low_u)
                hid[c * STEP_SUBS + s] = (g * jax.nn.sigmoid(g) * u).astype(BF)
        h = jnp.concatenate([hid[c * STEP_SUBS + s] for s in range(STEP_SUBS)], axis=1)
        low_d[...] += nn(h, ad_t[...])

        @pl.when(c + RING < n_steps)
        def _():
            start_ring(c + RING, range(len(whole)))

        for back in (0, 1):
            @pl.when(c == n_steps - 3 + back)
            def _(back=back):
                for j in range(3 * back, 3 * back + 3):
                    start_wd(j)

        return carry

    lax.fori_loop(0, n_steps, ff_step, 0)

    low_dm = jnp.where(own(), low_d[...], 0.0).astype(BF)
    low_g[...] = low_dm
    b_copy.wait()

    def back_copy(j, n, p):
        return pltpu.make_async_remote_copy(src_ref=ret.at[pl.ds(j, n), p], dst_ref=got.at[pl.ds(j, n), me], send_sem=rs_sem, recv_sem=rr_sem.at[j],
                                            device_id={"data": p}, device_id_type=pl.DeviceIdType.MESH)

    def columns(j, n):
        with jax.named_scope('wd_wait'):
            for k in range(n):
                landing(big.at[pl.ds(wd_at(j + k), fold), :], wd_sem.at[j + k]).wait()
        col = pl.ds(pl.multiple_of(j * SUB, 128), n * SUB)
        full = nn(low_g[...], b_buf[:, col])
        h = jnp.concatenate([hid[s] for s in range(ff // SUB)], axis=1)
        w = jnp.concatenate([jnp.concatenate([big[pl.ds(wd_at(j + k), fold), pl.ds(q * SUB, SUB)] for q in range(STEP_SUBS)], axis=0) for k in range(n)], axis=1)
        done = rows[:, col].astype(F32) + (nn(h, w) + (scale * full).astype(BF).astype(F32))
        for k in range(n):
            ret[j + k] = done[:, k * SUB:(k + 1) * SUB].reshape(groups, cap, SUB).astype(BF)
        for p in peers:
            back_copy(j, n, p).start()
        for k in range(n):
            got[j + k, me] = ret[j + k, me]

    def pair_step(i, carry):
        columns(2 * i + 1, 2)
        return carry

    columns(0, 1)
    lax.fori_loop(0, PAIRS, pair_step, 0)
    columns(cols - 1, 1)

    to_tok = (lax.broadcasted_iota(jnp.int32, (toks, slots), 1) == own_col * cap + arr_col).astype(F32).astype(BF)
    for j, n in [(0, 1)] + [(2 * i + 1, 2) for i in range(PAIRS)] + [(cols - 1, 1)]:
        with jax.named_scope('back_wait'):
            landing(got.at[pl.ds(j, n), :groups - 1], rr_sem.at[j]).wait()
        for k in range(j, j + n):
            block = got[k].astype(F32).reshape(slots, SUB).astype(BF)
            out_ref[:, k * SUB:(k + 1) * SUB] = nn(to_tok, block).astype(BF)
    with jax.named_scope('send_wait'):
        for p in peers:
            id_copy(p, p).wait_send()
        landing(send.at[:groups - 1], out_sem).wait()
        landing(ret.at[:, :groups - 1], rs_sem).wait()


def solution(mesh):
    groups = mesh.shape["data"]
    row_spec = P(("rep", "data"), None)
    id_spec = P(("rep", "data"))
    owned_spec = P("data", None, None)

    def device_step(x, adapter_id, w_gate, w_up, w_down, a_gate, b_gate, a_up, b_up, a_down, b_down):
        toks, width = x.shape
        per_owner, rank, ff = b_gate.shape
        ranks = per_owner * rank
        cap = (3 * toks + groups - 1) // groups
        slots = groups * cap
        cols = width // SUB
        ring_rows = 2 * width + 3 * ranks

        def flat(m):
            return m.reshape(ranks, m.shape[-1])

        return pl.pallas_call(
            functools.partial(layer_kernel, groups, rank, cap, per_owner),
            out_shape=pltpu.VMEM((toks, width), BF),
            in_specs=[pl.BlockSpec(memory_space=pltpu.VMEM)] * 2 + [pl.BlockSpec(memory_space=pl.ANY)] * 9,
            out_specs=pl.BlockSpec(memory_space=pltpu.VMEM),
            scratch_shapes=[
                pltpu.VMEM((groups, cap, width), BF),
                pltpu.VMEM((groups, cap, width), BF),
                pltpu.VMEM((slots, width), BF),
                pltpu.VMEM((slots, ranks), BF),
                pltpu.VMEM((slots, ranks), BF),
                pltpu.VMEM((ff // SUB, slots, SUB), BF),
                pltpu.VMEM((slots, ranks), F32),
                pltpu.VMEM((cols, groups, cap, SUB), BF),
                pltpu.VMEM((cols, groups, cap, SUB), BF),
                pltpu.VMEM((ranks, width), BF),
                pltpu.VMEM((STEP_SUBS * SUB, ranks), BF),
                pltpu.VMEM((RING * ring_rows, STEP_SUBS * SUB), BF),
                pltpu.VMEM((groups, 1, toks), jnp.int32),
                pltpu.VMEM((slots, 1), jnp.int32),
                pltpu.SemaphoreType.DMA((RING, len(GROUPS))),
                pltpu.SemaphoreType.DMA((2,)),
                pltpu.SemaphoreType.DMA,
                pltpu.SemaphoreType.DMA((cols,)),
                pltpu.SemaphoreType.DMA,
                pltpu.SemaphoreType.DMA,
                pltpu.SemaphoreType.DMA,
                pltpu.SemaphoreType.DMA((cols,)),
                pltpu.SemaphoreType.DMA,
                pltpu.SemaphoreType.DMA((groups,)),
            ],
            compiler_params=pltpu.CompilerParams(collective_id=0, has_side_effects=True, vmem_limit_bytes=66_400_000),
            name="lora_layer",
        )(x, adapter_id.reshape(1, toks), w_gate, w_up, w_down, flat(a_gate), flat(a_up), flat(b_gate), flat(b_up), flat(a_down), flat(b_down))

    return jax.shard_map(device_step, mesh=mesh, in_specs=(row_spec, id_spec, P(), P(), P(), owned_spec, owned_spec, owned_spec, owned_spec, owned_spec, owned_spec), out_specs=row_spec, check_vma=False)
```

```python
import functools

import jax
import jax.numpy as jnp
from jax import lax
from jax.experimental import pallas as pl
from jax.experimental.pallas import tpu as pltpu
from jax.sharding import PartitionSpec as P

ALPHA = 32
SUB = 256
STEP_SUBS = 5
RING = 3
GROUPS = ((0, 5),)
PAIRS = 2
BF = jnp.bfloat16
F32 = jnp.float32


def nn(a, b):
    return jnp.dot(a, b, preferred_element_type=F32)


def nt(a, b):
    return lax.dot_general(a, b, (((1,), (1,)), ((), ())), preferred_element_type=F32)


def count_ge(v, width, groups):
    total = jnp.zeros(v.shape, jnp.int32)
    for g in range(1, groups):
        total += (v >= g * width).astype(jnp.int32)
    return total


def layer_kernel(groups, rank, cap, per_owner, x_hbm, ids_hbm, wg, wu, wd, ag, au, bg, bu, ad, bd, out_ref,
                 send, recv, rows, low_g, low_u, hid, low_d, ret, got, b_buf, ad_t, big, all_ids, first, x_ref, ids_ref,
                 ring_sem, a_sem, b_sem, wd_sem, out_sem, in_sem, rs_sem, rr_sem, x_sem, id_out, id_in):
    toks, width = x_hbm.shape
    ff = wg.shape[1]
    ranks = per_owner * rank
    slots = groups * cap
    scale = ALPHA / rank
    step = STEP_SUBS * SUB
    n_steps = ff // step
    ring_rows = 2 * width + 3 * ranks
    fold = ff // STEP_SUBS
    cols = width // SUB
    whole = ((wg, 0, width), (wu, width, width), (bg, 2 * width, ranks), (bu, 2 * width + ranks, ranks), (ad, 2 * width + 2 * ranks, ranks))
    me = lax.axis_index("data")
    peers = [lax.rem(me + k, groups) for k in (4, 3, 5, 2, 6, 1, 7) if k < groups]

    def ring_copy(c, g, i):
        src, off, n = whole[i]
        lo, subs = GROUPS[g]
        slot = lax.rem(c, RING)
        start = pl.multiple_of(slot * ring_rows + off, 8)
        col = pl.multiple_of(c * step + lo * SUB, 128)
        return pltpu.make_async_copy(src.at[:, pl.ds(col, subs * SUB)], big.at[pl.ds(start, n), pl.ds(lo * SUB, subs * SUB)], ring_sem.at[slot, g])

    def start_ring(c, which):
        for g in range(len(GROUPS)):
            for i in which:
                ring_copy(c, g, i).start()

    def landing(dst, sem):
        return pltpu.make_async_copy(dst, dst, sem)

    def ring_wait(c, g):
        slot = lax.rem(c, RING)
        lo, subs = GROUPS[g]
        landing(big.at[pl.ds(pl.multiple_of(slot * ring_rows, 8), ring_rows), pl.ds(lo * SUB, subs * SUB)], ring_sem.at[slot, g]).wait()

    def wd_at(j):
        return pl.multiple_of(ring_rows * (1 + j // 3) + lax.rem(j, 3) * fold, 8)

    def wd_copy(j, q):
        col = pl.multiple_of(j * SUB, 128)
        return pltpu.make_async_copy(wd.at[pl.ds(q * fold, fold), pl.ds(col, SUB)], big.at[pl.ds(wd_at(j), fold), pl.ds(q * SUB, SUB)], wd_sem.at[j])

    def start_wd(j):
        for q in range(STEP_SUBS):
            wd_copy(j, q).start()

    rest = width - step
    barrier = pltpu.get_barrier_semaphore()
    for p in peers:
        pl.semaphore_signal(barrier, inc=1, device_id={"data": p}, device_id_type=pl.DeviceIdType.MESH)

    x_copies = [pltpu.make_async_copy(ids_hbm, ids_ref, x_sem.at[0]), pltpu.make_async_copy(x_hbm, x_ref, x_sem.at[1])]
    for cp in x_copies:
        cp.start()
    t_base = (RING - 1) * ring_rows
    a_base = t_base + 2 * width
    a_copies = []
    for i, src in enumerate((ag, au)):
        a_copies.append(pltpu.make_async_copy(src.at[:, :step], big.at[pl.ds(a_base + i * ranks, ranks), :], a_sem.at[i]))
        a_copies.append(pltpu.make_async_copy(src.at[:, step:], big.at[pl.ds(a_base + 2 * ranks, ranks), pl.ds(i * rest, rest)], a_sem.at[i]))
    b_copy = pltpu.make_async_copy(bd, b_buf, b_sem)
    for cp in a_copies:
        cp.start()
    for c in range(2):
        start_ring(c, range(len(whole)))
    b_copy.start()

    for cp in x_copies:
        cp.wait()
    id_row = ids_ref[...]
    sub_i = lax.broadcasted_iota(jnp.int32, (toks, toks), 0)
    lane_i = lax.broadcasted_iota(jnp.int32, (toks, toks), 1)
    id_col = jnp.sum(jnp.where(sub_i == lane_i, jnp.broadcast_to(id_row, (toks, toks)), 0), axis=1, keepdims=True)
    own_row = count_ge(id_row, per_owner, groups)
    own_col = count_ge(id_col, per_owner, groups)
    same = own_col == own_row
    arr_col = jnp.sum((same & (lane_i < sub_i)).astype(jnp.int32), axis=1, keepdims=True)
    arr_row = jnp.sum((same & (sub_i < lane_i)).astype(jnp.int32), axis=0, keepdims=True)
    to_slot = (lax.broadcasted_iota(jnp.int32, (slots, toks), 0) == own_row * cap + arr_row).astype(F32).astype(BF)
    send[...] = nn(to_slot, x_ref[...]).reshape(groups, cap, width).astype(BF)

    with jax.named_scope('entry_wait'):
        pl.semaphore_wait(barrier, groups - 1)

    def row_copy(p):
        return pltpu.make_async_remote_copy(src_ref=send.at[p], dst_ref=recv.at[me], send_sem=out_sem, recv_sem=in_sem,
                                            device_id={"data": p}, device_id_type=pl.DeviceIdType.MESH)

    def id_copy(p, at):
        return pltpu.make_async_remote_copy(src_ref=ids_ref, dst_ref=all_ids.at[at], send_sem=id_out, recv_sem=id_in.at[at],
                                            device_id={"data": p}, device_id_type=pl.DeviceIdType.MESH)

    for p in peers:
        id_copy(p, me).start()
    for p in peers:
        row_copy(p).start()
    all_ids[me] = ids_ref[...]
    recv[me] = send[me]
    for i in range(2):
        landing(b_buf, a_sem.at[i]).wait()
    for i in range(2):
        for r in range(0, ranks, 128):
            turned = pl.ds(r, 128)
            big[t_base + i * width:t_base + i * width + step, turned] = big[a_base + i * ranks + r:a_base + i * ranks + r + 128, :].T
            big[t_base + i * width + step:t_base + (i + 1) * width, turned] = big[a_base + 2 * ranks + r:a_base + 2 * ranks + r + 128, i * rest:(i + 1) * rest].T
    start_ring(RING - 1, range(2, len(whole)))
    for p in peers:
        id_copy(p, p).wait_recv()
    every = jnp.concatenate([all_ids[g] for g in range(groups)], axis=0)
    every = every - me * per_owner
    mine = ((every >= 0) & (every < per_owner)).astype(F32)
    before = nn(mine.astype(BF), (sub_i < lane_i).astype(F32).astype(BF))
    slot_i = lax.broadcasted_iota(jnp.int32, (cap, toks), 0).astype(F32)
    value = mine * (every * rank).astype(F32)
    first[...] = jnp.concatenate([jnp.sum(jnp.where(slot_i == before[g:g + 1, :], value[g:g + 1, :], 0.0), axis=1, keepdims=True) for g in range(groups)], axis=0).astype(jnp.int32)

    def own():
        rank_i = lax.broadcasted_iota(jnp.int32, (slots, ranks), 1)
        return (rank_i >= first[...]) & (rank_i < first[...] + rank)

    with jax.named_scope('row_wait'):
        landing(recv.at[:groups - 1], in_sem).wait()

    rows[...] = recv[...].astype(F32).reshape(slots, width).astype(BF)
    lows = [nn(rows[...], big[t_base + i * width:t_base + (i + 1) * width, :ranks]) for i in range(2)]
    low_g[...] = jnp.where(own(), lows[0], 0.0).astype(BF)
    low_u[...] = jnp.where(own(), lows[1], 0.0).astype(BF)
    start_ring(RING - 1, range(2))
    low_d[...] = jnp.zeros_like(low_d)

    def half(base, col, w_off, w_n, b_off, low):
        full = nn(low[...], big[pl.ds(base + b_off, ranks), col])
        return nn(rows[...], big[pl.ds(base + w_off, w_n), col]) + (scale * full).astype(BF).astype(F32)

    def ff_step(c, carry):
        base = pl.multiple_of(lax.rem(c, RING) * ring_rows, 8)
        for n, (lo, subs) in enumerate(GROUPS):
            with jax.named_scope('ring_wait'):
                ring_wait(c, n)
            for s in range(lo, lo + subs):
                col = pl.ds(s * SUB, SUB)
                ad_t[s * SUB:(s + 1) * SUB, :] = big[pl.ds(base + 2 * width + 2 * ranks, ranks), col].T
                g = half(base, col, 0, width, 2 * width, low_g)
                u = half(base, col, width, width, 2 * width + ranks, low_u)
                hid[c * STEP_SUBS + s] = (g * jax.nn.sigmoid(g) * u).astype(BF)
        h = jnp.concatenate([hid[c * STEP_SUBS + s] for s in range(STEP_SUBS)], axis=1)
        low_d[...] += nn(h, ad_t[...])

        @pl.when(c + RING < n_steps)
        def _():
            start_ring(c + RING, range(len(whole)))

        for back in (0, 1):
            @pl.when(c == n_steps - 3 + back)
            def _(back=back):
                for j in range(3 * back, 3 * back + 3):
                    start_wd(j)

        return carry

    lax.fori_loop(0, n_steps, ff_step, 0)

    low_dm = jnp.where(own(), low_d[...], 0.0).astype(BF)
    low_g[...] = low_dm
    b_copy.wait()

    def back_copy(j, n, p):
        return pltpu.make_async_remote_copy(src_ref=ret.at[pl.ds(j, n), p], dst_ref=got.at[pl.ds(j, n), me], send_sem=rs_sem, recv_sem=rr_sem.at[j],
                                            device_id={"data": p}, device_id_type=pl.DeviceIdType.MESH)

    def columns(j, n):
        with jax.named_scope('wd_wait'):
            for k in range(n):
                landing(big.at[pl.ds(wd_at(j + k), fold), :], wd_sem.at[j + k]).wait()
        col = pl.ds(pl.multiple_of(j * SUB, 128), n * SUB)
        full = nn(low_g[...], b_buf[:, col])
        h = jnp.concatenate([hid[s] for s in range(ff // SUB)], axis=1)
        w = jnp.concatenate([jnp.concatenate([big[pl.ds(wd_at(j + k), fold), pl.ds(q * SUB, SUB)] for q in range(STEP_SUBS)], axis=0) for k in range(n)], axis=1)
        done = rows[:, col].astype(F32) + (nn(h, w) + (scale * full).astype(BF).astype(F32))
        for k in range(n):
            ret[j + k] = done[:, k * SUB:(k + 1) * SUB].reshape(groups, cap, SUB).astype(BF)
        for p in peers:
            back_copy(j, n, p).start()
        for k in range(n):
            got[j + k, me] = ret[j + k, me]

    def pair_step(i, carry):
        columns(2 * i + 1, 2)
        return carry

    columns(0, 1)
    lax.fori_loop(0, PAIRS, pair_step, 0)
    columns(cols - 1, 1)

    to_tok = (lax.broadcasted_iota(jnp.int32, (toks, slots), 1) == own_col * cap + arr_col).astype(F32).astype(BF)
    for j, n in [(0, 1)] + [(2 * i + 1, 2) for i in range(PAIRS)] + [(cols - 1, 1)]:
        with jax.named_scope('back_wait'):
            landing(got.at[pl.ds(j, n), :groups - 1], rr_sem.at[j]).wait()
        for k in range(j, j + n):
            block = got[k].astype(F32).reshape(slots, SUB).astype(BF)
            out_ref[:, k * SUB:(k + 1) * SUB] = nn(to_tok, block).astype(BF)
    with jax.named_scope('send_wait'):
        for p in peers:
            id_copy(p, p).wait_send()
        landing(send.at[:groups - 1], out_sem).wait()
        landing(ret.at[:, :groups - 1], rs_sem).wait()


def solution(mesh):
    groups = mesh.shape["data"]
    row_spec = P(("rep", "data"), None)
    id_spec = P(("rep", "data"))
    owned_spec = P("data", None, None)

    def device_step(x, adapter_id, w_gate, w_up, w_down, a_gate, b_gate, a_up, b_up, a_down, b_down):
        toks, width = x.shape
        per_owner, rank, ff = b_gate.shape
        ranks = per_owner * rank
        cap = (3 * toks + groups - 1) // groups
        slots = groups * cap
        cols = width // SUB
        ring_rows = 2 * width + 3 * ranks

        def flat(m):
            return m.reshape(ranks, m.shape[-1])

        return pl.pallas_call(
            functools.partial(layer_kernel, groups, rank, cap, per_owner),
            out_shape=pltpu.VMEM((toks, width), BF),
            in_specs=[pl.BlockSpec(memory_space=pl.ANY)] * 11,
            out_specs=pl.BlockSpec(memory_space=pltpu.VMEM),
            scratch_shapes=[
                pltpu.VMEM((groups, cap, width), BF),
                pltpu.VMEM((groups, cap, width), BF),
                pltpu.VMEM((slots, width), BF),
                pltpu.VMEM((slots, ranks), BF),
                pltpu.VMEM((slots, ranks), BF),
                pltpu.VMEM((ff // SUB, slots, SUB), BF),
                pltpu.VMEM((slots, ranks), F32),
                pltpu.VMEM((cols, groups, cap, SUB), BF),
                pltpu.VMEM((cols, groups, cap, SUB), BF),
                pltpu.VMEM((ranks, width), BF),
                pltpu.VMEM((STEP_SUBS * SUB, ranks), BF),
                pltpu.VMEM((RING * ring_rows, STEP_SUBS * SUB), BF),
                pltpu.VMEM((groups, 1, toks), jnp.int32),
                pltpu.VMEM((slots, 1), jnp.int32),
                pltpu.VMEM((toks, width), BF),
                pltpu.VMEM((1, toks), jnp.int32),
                pltpu.SemaphoreType.DMA((RING, len(GROUPS))),
                pltpu.SemaphoreType.DMA((2,)),
                pltpu.SemaphoreType.DMA,
                pltpu.SemaphoreType.DMA((cols,)),
                pltpu.SemaphoreType.DMA,
                pltpu.SemaphoreType.DMA,
                pltpu.SemaphoreType.DMA,
                pltpu.SemaphoreType.DMA((cols,)),
                pltpu.SemaphoreType.DMA((2,)),
                pltpu.SemaphoreType.DMA,
                pltpu.SemaphoreType.DMA((groups,)),
            ],
            compiler_params=pltpu.CompilerParams(collective_id=0, has_side_effects=True, vmem_limit_bytes=66_400_000),
            name="lora_layer",
        )(x, adapter_id.reshape(1, toks), w_gate, w_up, w_down, flat(a_gate), flat(a_up), flat(b_gate), flat(b_up), flat(a_down), flat(b_down))

    return jax.shard_map(device_step, mesh=mesh, in_specs=(row_spec, id_spec, P(), P(), P(), owned_spec, owned_spec, owned_spec, owned_spec, owned_spec, owned_spec), out_specs=row_spec, check_vma=False)
```

```python
import functools

import jax
import jax.numpy as jnp
from jax import lax
from jax.experimental import pallas as pl
from jax.experimental.pallas import tpu as pltpu
from jax.sharding import PartitionSpec as P

ALPHA = 32
SUB = 256
STEP_SUBS = 5
RING = 3
CUT = 512
PAIRS = 2
BF = jnp.bfloat16
F32 = jnp.float32


def nn(a, b):
    return jnp.dot(a, b, preferred_element_type=F32)


def nt(a, b):
    return lax.dot_general(a, b, (((1,), (1,)), ((), ())), preferred_element_type=F32)


def count_ge(v, width, groups):
    total = jnp.zeros(v.shape, jnp.int32)
    for g in range(1, groups):
        total += (v >= g * width).astype(jnp.int32)
    return total


def layer_kernel(groups, rank, cap, per_owner, x_hbm, ids_hbm, wg, wu, wd, ag, au, bg, bu, ad, bd, out_ref,
                 send, recv, rows, low_g, low_u, hid, low_d, ret, got, b_buf, ad_t, big, all_ids, first, x_ref, ids_ref,
                 ring_sem, a_sem, b_sem, wd_sem, out_sem, in_sem, rs_sem, rr_sem, x_sem, id_out, id_in):
    toks, width = x_hbm.shape
    ff = wg.shape[1]
    ranks = per_owner * rank
    slots = groups * cap
    scale = ALPHA / rank
    step = STEP_SUBS * SUB
    n_steps = ff // step
    ring_rows = 2 * width + 3 * ranks
    fold = ff // STEP_SUBS
    cols = width // SUB
    whole = ((wg, 0, width), (wu, width, width), (bg, 2 * width, ranks), (bu, 2 * width + ranks, ranks), (ad, 2 * width + 2 * ranks, ranks))
    me = lax.axis_index("data")
    peers = [lax.rem(me + k, groups) for k in (4, 3, 5, 2, 6, 1, 7) if k < groups]

    def start_ring(c, which):
        slot = lax.rem(c, RING)
        col = pl.multiple_of(c * step, 128)
        for i in which:
            src, off, n = whole[i]
            for row in range(0, n, CUT):
                at = pl.multiple_of(slot * ring_rows + off + row, 8)
                pltpu.make_async_copy(src.at[pl.ds(row, CUT), pl.ds(col, step)], big.at[pl.ds(at, CUT), :], ring_sem.at[slot]).start()

    def landing(dst, sem):
        return pltpu.make_async_copy(dst, dst, sem)

    def ring_wait(c):
        slot = lax.rem(c, RING)
        landing(big.at[pl.ds(pl.multiple_of(slot * ring_rows, 8), ring_rows), :], ring_sem.at[slot]).wait()

    def wd_at(j):
        return pl.multiple_of(ring_rows * (1 + j // 3) + lax.rem(j, 3) * fold, 8)

    def wd_copy(j, q):
        col = pl.multiple_of(j * SUB, 128)
        return pltpu.make_async_copy(wd.at[pl.ds(q * fold, fold), pl.ds(col, SUB)], big.at[pl.ds(wd_at(j), fold), pl.ds(q * SUB, SUB)], wd_sem.at[j])

    def start_wd(j):
        for q in range(STEP_SUBS):
            wd_copy(j, q).start()

    rest = width - step
    x_copies = [pltpu.make_async_copy(ids_hbm, ids_ref, x_sem.at[0]), pltpu.make_async_copy(x_hbm, x_ref, x_sem.at[1])]
    for cp in x_copies:
        cp.start()
    barrier = pltpu.get_barrier_semaphore()
    for p in peers:
        pl.semaphore_signal(barrier, inc=1, device_id={"data": p}, device_id_type=pl.DeviceIdType.MESH)

    t_base = (RING - 1) * ring_rows
    a_base = t_base + 2 * width
    a_copies = []
    for i, src in enumerate((ag, au)):
        a_copies.append(pltpu.make_async_copy(src.at[:, :step], big.at[pl.ds(a_base + i * ranks, ranks), :], a_sem.at[i]))
        a_copies.append(pltpu.make_async_copy(src.at[:, step:], big.at[pl.ds(a_base + 2 * ranks, ranks), pl.ds(i * rest, rest)], a_sem.at[i]))
    b_copy = pltpu.make_async_copy(bd, b_buf, b_sem)
    for cp in a_copies:
        cp.start()
    for c in range(2):
        start_ring(c, range(len(whole)))
    b_copy.start()

    for cp in x_copies:
        cp.wait()
    id_row = ids_ref[...]
    sub_i = lax.broadcasted_iota(jnp.int32, (toks, toks), 0)
    lane_i = lax.broadcasted_iota(jnp.int32, (toks, toks), 1)
    id_col = jnp.sum(jnp.where(sub_i == lane_i, jnp.broadcast_to(id_row, (toks, toks)), 0), axis=1, keepdims=True)
    own_row = count_ge(id_row, per_owner, groups)
    own_col = count_ge(id_col, per_owner, groups)
    same = own_col == own_row
    arr_col = jnp.sum((same & (lane_i < sub_i)).astype(jnp.int32), axis=1, keepdims=True)
    arr_row = jnp.sum((same & (sub_i < lane_i)).astype(jnp.int32), axis=0, keepdims=True)
    to_slot = (lax.broadcasted_iota(jnp.int32, (slots, toks), 0) == own_row * cap + arr_row).astype(F32).astype(BF)
    send[...] = nn(to_slot, x_ref[...]).reshape(groups, cap, width).astype(BF)

    with jax.named_scope('entry_wait'):
        pl.semaphore_wait(barrier, groups - 1)

    def row_copy(p):
        return pltpu.make_async_remote_copy(src_ref=send.at[p], dst_ref=recv.at[me], send_sem=out_sem, recv_sem=in_sem,
                                            device_id={"data": p}, device_id_type=pl.DeviceIdType.MESH)

    def id_copy(p, at):
        return pltpu.make_async_remote_copy(src_ref=ids_ref, dst_ref=all_ids.at[at], send_sem=id_out, recv_sem=id_in.at[at],
                                            device_id={"data": p}, device_id_type=pl.DeviceIdType.MESH)

    for p in peers:
        id_copy(p, me).start()
    for p in peers:
        row_copy(p).start()
    all_ids[me] = ids_ref[...]
    recv[me] = send[me]
    for i in range(2):
        landing(b_buf, a_sem.at[i]).wait()
    for i in range(2):
        for r in range(0, ranks, 128):
            turned = pl.ds(r, 128)
            big[t_base + i * width:t_base + i * width + step, turned] = big[a_base + i * ranks + r:a_base + i * ranks + r + 128, :].T
            big[t_base + i * width + step:t_base + (i + 1) * width, turned] = big[a_base + 2 * ranks + r:a_base + 2 * ranks + r + 128, i * rest:(i + 1) * rest].T
    start_ring(RING - 1, range(2, len(whole)))
    for p in peers:
        id_copy(p, p).wait_recv()
    every = jnp.concatenate([all_ids[g] for g in range(groups)], axis=0)
    every = every - me * per_owner
    mine = ((every >= 0) & (every < per_owner)).astype(F32)
    before = nn(mine.astype(BF), (sub_i < lane_i).astype(F32).astype(BF))
    slot_i = lax.broadcasted_iota(jnp.int32, (cap, toks), 0).astype(F32)
    value = mine * (every * rank).astype(F32)
    first[...] = jnp.concatenate([jnp.sum(jnp.where(slot_i == before[g:g + 1, :], value[g:g + 1, :], 0.0), axis=1, keepdims=True) for g in range(groups)], axis=0).astype(jnp.int32)

    def own():
        rank_i = lax.broadcasted_iota(jnp.int32, (slots, ranks), 1)
        return (rank_i >= first[...]) & (rank_i < first[...] + rank)

    with jax.named_scope('row_wait'):
        landing(recv.at[:groups - 1], in_sem).wait()

    rows[...] = recv[...].astype(F32).reshape(slots, width).astype(BF)
    lows = [nn(rows[...], big[t_base + i * width:t_base + (i + 1) * width, :ranks]) for i in range(2)]
    low_g[...] = jnp.where(own(), lows[0], 0.0).astype(BF)
    low_u[...] = jnp.where(own(), lows[1], 0.0).astype(BF)
    start_ring(RING - 1, range(2))
    low_d[...] = jnp.zeros_like(low_d)

    def half(base, col, w_off, w_n, b_off, low):
        full = nn(low[...], big[pl.ds(base + b_off, ranks), col])
        return nn(rows[...], big[pl.ds(base + w_off, w_n), col]) + (scale * full).astype(BF).astype(F32)

    def ff_step(c, carry):
        base = pl.multiple_of(lax.rem(c, RING) * ring_rows, 8)
        with jax.named_scope('ring_wait'):
            ring_wait(c)
        for s in range(STEP_SUBS):
            col = pl.ds(s * SUB, SUB)
            ad_t[s * SUB:(s + 1) * SUB, :] = big[pl.ds(base + 2 * width + 2 * ranks, ranks), col].T
            g = half(base, col, 0, width, 2 * width, low_g)
            u = half(base, col, width, width, 2 * width + ranks, low_u)
            hid[c * STEP_SUBS + s] = (g * jax.nn.sigmoid(g) * u).astype(BF)
        h = jnp.concatenate([hid[c * STEP_SUBS + s] for s in range(STEP_SUBS)], axis=1)
        low_d[...] += nn(h, ad_t[...])

        @pl.when(c + RING < n_steps)
        def _():
            start_ring(c + RING, range(len(whole)))

        for back in (0, 1):
            @pl.when(c == n_steps - 3 + back)
            def _(back=back):
                for j in range(3 * back, 3 * back + 3):
                    start_wd(j)

        return carry

    lax.fori_loop(0, n_steps, ff_step, 0)

    low_dm = jnp.where(own(), low_d[...], 0.0).astype(BF)
    low_g[...] = low_dm
    b_copy.wait()

    def back_copy(j, n, p):
        return pltpu.make_async_remote_copy(src_ref=ret.at[pl.ds(j, n), p], dst_ref=got.at[pl.ds(j, n), me], send_sem=rs_sem, recv_sem=rr_sem.at[j],
                                            device_id={"data": p}, device_id_type=pl.DeviceIdType.MESH)

    def columns(j, n):
        with jax.named_scope('wd_wait'):
            for k in range(n):
                landing(big.at[pl.ds(wd_at(j + k), fold), :], wd_sem.at[j + k]).wait()
        col = pl.ds(pl.multiple_of(j * SUB, 128), n * SUB)
        full = nn(low_g[...], b_buf[:, col])
        h = jnp.concatenate([hid[s] for s in range(ff // SUB)], axis=1)
        w = jnp.concatenate([jnp.concatenate([big[pl.ds(wd_at(j + k), fold), pl.ds(q * SUB, SUB)] for q in range(STEP_SUBS)], axis=0) for k in range(n)], axis=1)
        done = rows[:, col].astype(F32) + (nn(h, w) + (scale * full).astype(BF).astype(F32))
        for k in range(n):
            ret[j + k] = done[:, k * SUB:(k + 1) * SUB].reshape(groups, cap, SUB).astype(BF)
        for p in peers:
            back_copy(j, n, p).start()
        for k in range(n):
            got[j + k, me] = ret[j + k, me]

    def pair_step(i, carry):
        columns(2 * i + 1, 2)
        return carry

    columns(0, 1)
    lax.fori_loop(0, PAIRS, pair_step, 0)
    columns(cols - 1, 1)

    to_tok = (lax.broadcasted_iota(jnp.int32, (toks, slots), 1) == own_col * cap + arr_col).astype(F32).astype(BF)
    for j, n in [(0, 1)] + [(2 * i + 1, 2) for i in range(PAIRS)] + [(cols - 1, 1)]:
        with jax.named_scope('back_wait'):
            landing(got.at[pl.ds(j, n), :groups - 1], rr_sem.at[j]).wait()
        for k in range(j, j + n):
            block = got[k].astype(F32).reshape(slots, SUB).astype(BF)
            out_ref[:, k * SUB:(k + 1) * SUB] = nn(to_tok, block).astype(BF)
    with jax.named_scope('send_wait'):
        for p in peers:
            id_copy(p, p).wait_send()
        landing(send.at[:groups - 1], out_sem).wait()
        landing(ret.at[:, :groups - 1], rs_sem).wait()


def solution(mesh):
    groups = mesh.shape["data"]
    row_spec = P(("rep", "data"), None)
    id_spec = P(("rep", "data"))
    owned_spec = P("data", None, None)

    def device_step(x, adapter_id, w_gate, w_up, w_down, a_gate, b_gate, a_up, b_up, a_down, b_down):
        toks, width = x.shape
        per_owner, rank, ff = b_gate.shape
        ranks = per_owner * rank
        cap = (3 * toks + groups - 1) // groups
        slots = groups * cap
        cols = width // SUB
        ring_rows = 2 * width + 3 * ranks

        def flat(m):
            return m.reshape(ranks, m.shape[-1])

        return pl.pallas_call(
            functools.partial(layer_kernel, groups, rank, cap, per_owner),
            out_shape=pltpu.VMEM((toks, width), BF),
            in_specs=[pl.BlockSpec(memory_space=pl.ANY)] * 11,
            out_specs=pl.BlockSpec(memory_space=pltpu.VMEM),
            scratch_shapes=[
                pltpu.VMEM((groups, cap, width), BF),
                pltpu.VMEM((groups, cap, width), BF),
                pltpu.VMEM((slots, width), BF),
                pltpu.VMEM((slots, ranks), BF),
                pltpu.VMEM((slots, ranks), BF),
                pltpu.VMEM((ff // SUB, slots, SUB), BF),
                pltpu.VMEM((slots, ranks), F32),
                pltpu.VMEM((cols, groups, cap, SUB), BF),
                pltpu.VMEM((cols, groups, cap, SUB), BF),
                pltpu.VMEM((ranks, width), BF),
                pltpu.VMEM((STEP_SUBS * SUB, ranks), BF),
                pltpu.VMEM((RING * ring_rows, STEP_SUBS * SUB), BF),
                pltpu.VMEM((groups, 1, toks), jnp.int32),
                pltpu.VMEM((slots, 1), jnp.int32),
                pltpu.VMEM((toks, width), BF),
                pltpu.VMEM((1, toks), jnp.int32),
                pltpu.SemaphoreType.DMA((RING,)),
                pltpu.SemaphoreType.DMA((2,)),
                pltpu.SemaphoreType.DMA,
                pltpu.SemaphoreType.DMA((cols,)),
                pltpu.SemaphoreType.DMA,
                pltpu.SemaphoreType.DMA,
                pltpu.SemaphoreType.DMA,
                pltpu.SemaphoreType.DMA((cols,)),
                pltpu.SemaphoreType.DMA((2,)),
                pltpu.SemaphoreType.DMA,
                pltpu.SemaphoreType.DMA((groups,)),
            ],
            compiler_params=pltpu.CompilerParams(collective_id=0, has_side_effects=True, vmem_limit_bytes=66_400_000),
            name="lora_layer",
        )(x, adapter_id.reshape(1, toks), w_gate, w_up, w_down, flat(a_gate), flat(a_up), flat(b_gate), flat(b_up), flat(a_down), flat(b_down))

    return jax.shard_map(device_step, mesh=mesh, in_specs=(row_spec, id_spec, P(), P(), P(), owned_spec, owned_spec, owned_spec, owned_spec, owned_spec, owned_spec), out_specs=row_spec, check_vma=False)
```

```python
import functools

import jax
import jax.numpy as jnp
from jax import lax
from jax.experimental import pallas as pl
from jax.experimental.pallas import tpu as pltpu
from jax.sharding import PartitionSpec as P

ALPHA = 32
SUB = 256
STEP_SUBS = 5
RING = 3
GROUPS = ((0, 3), (3, 2))
PAIRS = 2
BF = jnp.bfloat16
F32 = jnp.float32


def nn(a, b):
    return jnp.dot(a, b, preferred_element_type=F32)


def nt(a, b):
    return lax.dot_general(a, b, (((1,), (1,)), ((), ())), preferred_element_type=F32)


def count_ge(v, width, groups):
    total = jnp.zeros(v.shape, jnp.int32)
    for g in range(1, groups):
        total += (v >= g * width).astype(jnp.int32)
    return total


def layer_kernel(groups, rank, cap, per_owner, x_hbm, ids_hbm, wg, wu, wd, ag, au, bg, bu, ad, bd, out_ref,
                 send, recv, rows, low_g, low_u, hid, low_d, ret, got, b_buf, ad_t, big, all_ids, first, x_ref, ids_ref,
                 ring_sem, a_sem, b_sem, wd_sem, out_sem, in_sem, rs_sem, rr_sem, x_sem, id_out, id_in):
    toks, width = x_hbm.shape
    ff = wg.shape[1]
    ranks = per_owner * rank
    slots = groups * cap
    scale = ALPHA / rank
    step = STEP_SUBS * SUB
    n_steps = ff // step
    ring_rows = 2 * width + 3 * ranks
    fold = ff // STEP_SUBS
    cols = width // SUB
    whole = ((wg, 0, width), (wu, width, width), (bg, 2 * width, ranks), (bu, 2 * width + ranks, ranks), (ad, 2 * width + 2 * ranks, ranks))
    me = lax.axis_index("data")
    peers = [lax.rem(me + k, groups) for k in (4, 3, 5, 2, 6, 1, 7) if k < groups]

    def start_ring(c, which):
        slot = lax.rem(c, RING)
        for k, (lo, subs) in enumerate(GROUPS):
            col = pl.multiple_of(c * step + lo * SUB, 128)
            for i in which:
                src, off, n = whole[i]
                at = pl.multiple_of(slot * ring_rows + off, 8)
                pltpu.make_async_copy(src.at[:, pl.ds(col, subs * SUB)], big.at[pl.ds(at, n), pl.ds(lo * SUB, subs * SUB)], ring_sem.at[slot, k]).start()

    def landing(dst, sem):
        return pltpu.make_async_copy(dst, dst, sem)

    def ring_wait(c, k):
        slot = lax.rem(c, RING)
        lo, subs = GROUPS[k]
        landing(big.at[pl.ds(pl.multiple_of(slot * ring_rows, 8), ring_rows), pl.ds(lo * SUB, subs * SUB)], ring_sem.at[slot, k]).wait()

    def wd_at(j):
        return pl.multiple_of(ring_rows * (1 + j // 3) + lax.rem(j, 3) * fold, 8)

    def wd_copy(j, q):
        col = pl.multiple_of(j * SUB, 128)
        return pltpu.make_async_copy(wd.at[pl.ds(q * fold, fold), pl.ds(col, SUB)], big.at[pl.ds(wd_at(j), fold), pl.ds(q * SUB, SUB)], wd_sem.at[j])

    def start_wd(j):
        for q in range(STEP_SUBS):
            wd_copy(j, q).start()

    rest = width - step
    x_copies = [pltpu.make_async_copy(ids_hbm, ids_ref, x_sem.at[0]), pltpu.make_async_copy(x_hbm, x_ref, x_sem.at[1])]
    for cp in x_copies:
        cp.start()
    barrier = pltpu.get_barrier_semaphore()
    for p in peers:
        pl.semaphore_signal(barrier, inc=1, device_id={"data": p}, device_id_type=pl.DeviceIdType.MESH)

    t_base = (RING - 1) * ring_rows
    a_base = t_base + 2 * width
    a_copies = []
    for i, src in enumerate((ag, au)):
        a_copies.append(pltpu.make_async_copy(src.at[:, :step], big.at[pl.ds(a_base + i * ranks, ranks), :], a_sem.at[i]))
        a_copies.append(pltpu.make_async_copy(src.at[:, step:], big.at[pl.ds(a_base + 2 * ranks, ranks), pl.ds(i * rest, rest)], a_sem.at[i]))
    b_copy = pltpu.make_async_copy(bd, b_buf, b_sem)
    for cp in a_copies:
        cp.start()
    for c in range(2):
        start_ring(c, range(len(whole)))
    b_copy.start()

    for cp in x_copies:
        cp.wait()
    id_row = ids_ref[...]
    sub_i = lax.broadcasted_iota(jnp.int32, (toks, toks), 0)
    lane_i = lax.broadcasted_iota(jnp.int32, (toks, toks), 1)
    id_col = jnp.sum(jnp.where(sub_i == lane_i, jnp.broadcast_to(id_row, (toks, toks)), 0), axis=1, keepdims=True)
    own_row = count_ge(id_row, per_owner, groups)
    own_col = count_ge(id_col, per_owner, groups)
    same = own_col == own_row
    arr_col = jnp.sum((same & (lane_i < sub_i)).astype(jnp.int32), axis=1, keepdims=True)
    arr_row = jnp.sum((same & (sub_i < lane_i)).astype(jnp.int32), axis=0, keepdims=True)
    to_slot = (lax.broadcasted_iota(jnp.int32, (slots, toks), 0) == own_row * cap + arr_row).astype(F32).astype(BF)
    send[...] = nn(to_slot, x_ref[...]).reshape(groups, cap, width).astype(BF)

    with jax.named_scope('entry_wait'):
        pl.semaphore_wait(barrier, groups - 1)

    def row_copy(p):
        return pltpu.make_async_remote_copy(src_ref=send.at[p], dst_ref=recv.at[me], send_sem=out_sem, recv_sem=in_sem,
                                            device_id={"data": p}, device_id_type=pl.DeviceIdType.MESH)

    def id_copy(p, at):
        return pltpu.make_async_remote_copy(src_ref=ids_ref, dst_ref=all_ids.at[at], send_sem=id_out, recv_sem=id_in.at[at],
                                            device_id={"data": p}, device_id_type=pl.DeviceIdType.MESH)

    for p in peers:
        id_copy(p, me).start()
    for p in peers:
        row_copy(p).start()
    all_ids[me] = ids_ref[...]
    recv[me] = send[me]
    for i in range(2):
        landing(b_buf, a_sem.at[i]).wait()
    for i in range(2):
        for r in range(0, ranks, 128):
            turned = pl.ds(r, 128)
            big[t_base + i * width:t_base + i * width + step, turned] = big[a_base + i * ranks + r:a_base + i * ranks + r + 128, :].T
            big[t_base + i * width + step:t_base + (i + 1) * width, turned] = big[a_base + 2 * ranks + r:a_base + 2 * ranks + r + 128, i * rest:(i + 1) * rest].T
    start_ring(RING - 1, range(2, len(whole)))
    for p in peers:
        id_copy(p, p).wait_recv()
    every = jnp.concatenate([all_ids[g] for g in range(groups)], axis=0)
    every = every - me * per_owner
    mine = ((every >= 0) & (every < per_owner)).astype(F32)
    before = nn(mine.astype(BF), (sub_i < lane_i).astype(F32).astype(BF))
    slot_i = lax.broadcasted_iota(jnp.int32, (cap, toks), 0).astype(F32)
    value = mine * (every * rank).astype(F32)
    first[...] = jnp.concatenate([jnp.sum(jnp.where(slot_i == before[g:g + 1, :], value[g:g + 1, :], 0.0), axis=1, keepdims=True) for g in range(groups)], axis=0).astype(jnp.int32)

    def own():
        rank_i = lax.broadcasted_iota(jnp.int32, (slots, ranks), 1)
        return (rank_i >= first[...]) & (rank_i < first[...] + rank)

    with jax.named_scope('row_wait'):
        landing(recv.at[:groups - 1], in_sem).wait()

    rows[...] = recv[...].astype(F32).reshape(slots, width).astype(BF)
    lows = [nn(rows[...], big[t_base + i * width:t_base + (i + 1) * width, :ranks]) for i in range(2)]
    low_g[...] = jnp.where(own(), lows[0], 0.0).astype(BF)
    low_u[...] = jnp.where(own(), lows[1], 0.0).astype(BF)
    start_ring(RING - 1, range(2))
    low_d[...] = jnp.zeros_like(low_d)

    def half(base, col, w_off, w_n, b_off, low):
        full = nn(low[...], big[pl.ds(base + b_off, ranks), col])
        return nn(rows[...], big[pl.ds(base + w_off, w_n), col]) + (scale * full).astype(BF).astype(F32)

    def ff_step(c, carry):
        base = pl.multiple_of(lax.rem(c, RING) * ring_rows, 8)
        for k, (lo, subs) in enumerate(GROUPS):
            with jax.named_scope('ring_wait'):
                ring_wait(c, k)
            for s in range(lo, lo + subs):
                col = pl.ds(s * SUB, SUB)
                ad_t[s * SUB:(s + 1) * SUB, :] = big[pl.ds(base + 2 * width + 2 * ranks, ranks), col].T
                g = half(base, col, 0, width, 2 * width, low_g)
                u = half(base, col, width, width, 2 * width + ranks, low_u)
                hid[c * STEP_SUBS + s] = (g * jax.nn.sigmoid(g) * u).astype(BF)
        h = jnp.concatenate([hid[c * STEP_SUBS + s] for s in range(STEP_SUBS)], axis=1)
        low_d[...] += nn(h, ad_t[...])

        @pl.when(c + RING < n_steps)
        def _():
            start_ring(c + RING, range(len(whole)))

        for back in (0, 1):
            @pl.when(c == n_steps - 3 + back)
            def _(back=back):
                for j in range(3 * back, 3 * back + 3):
                    start_wd(j)

        return carry

    lax.fori_loop(0, n_steps, ff_step, 0)

    low_dm = jnp.where(own(), low_d[...], 0.0).astype(BF)
    low_g[...] = low_dm
    b_copy.wait()

    def back_copy(j, n, p):
        return pltpu.make_async_remote_copy(src_ref=ret.at[pl.ds(j, n), p], dst_ref=got.at[pl.ds(j, n), me], send_sem=rs_sem, recv_sem=rr_sem.at[j],
                                            device_id={"data": p}, device_id_type=pl.DeviceIdType.MESH)

    def columns(j, n):
        with jax.named_scope('wd_wait'):
            for k in range(n):
                landing(big.at[pl.ds(wd_at(j + k), fold), :], wd_sem.at[j + k]).wait()
        col = pl.ds(pl.multiple_of(j * SUB, 128), n * SUB)
        full = nn(low_g[...], b_buf[:, col])
        h = jnp.concatenate([hid[s] for s in range(ff // SUB)], axis=1)
        w = jnp.concatenate([jnp.concatenate([big[pl.ds(wd_at(j + k), fold), pl.ds(q * SUB, SUB)] for q in range(STEP_SUBS)], axis=0) for k in range(n)], axis=1)
        done = rows[:, col].astype(F32) + (nn(h, w) + (scale * full).astype(BF).astype(F32))
        for k in range(n):
            ret[j + k] = done[:, k * SUB:(k + 1) * SUB].reshape(groups, cap, SUB).astype(BF)
        for p in peers:
            back_copy(j, n, p).start()
        for k in range(n):
            got[j + k, me] = ret[j + k, me]

    def pair_step(i, carry):
        columns(2 * i + 1, 2)
        return carry

    columns(0, 1)
    lax.fori_loop(0, PAIRS, pair_step, 0)
    columns(cols - 1, 1)

    to_tok = (lax.broadcasted_iota(jnp.int32, (toks, slots), 1) == own_col * cap + arr_col).astype(F32).astype(BF)
    for j, n in [(0, 1)] + [(2 * i + 1, 2) for i in range(PAIRS)] + [(cols - 1, 1)]:
        with jax.named_scope('back_wait'):
            landing(got.at[pl.ds(j, n), :groups - 1], rr_sem.at[j]).wait()
        for k in range(j, j + n):
            block = got[k].astype(F32).reshape(slots, SUB).astype(BF)
            out_ref[:, k * SUB:(k + 1) * SUB] = nn(to_tok, block).astype(BF)
    with jax.named_scope('send_wait'):
        for p in peers:
            id_copy(p, p).wait_send()
        landing(send.at[:groups - 1], out_sem).wait()
        landing(ret.at[:, :groups - 1], rs_sem).wait()


def solution(mesh):
    groups = mesh.shape["data"]
    row_spec = P(("rep", "data"), None)
    id_spec = P(("rep", "data"))
    owned_spec = P("data", None, None)

    def device_step(x, adapter_id, w_gate, w_up, w_down, a_gate, b_gate, a_up, b_up, a_down, b_down):
        toks, width = x.shape
        per_owner, rank, ff = b_gate.shape
        ranks = per_owner * rank
        cap = (3 * toks + groups - 1) // groups
        slots = groups * cap
        cols = width // SUB
        ring_rows = 2 * width + 3 * ranks

        def flat(m):
            return m.reshape(ranks, m.shape[-1])

        return pl.pallas_call(
            functools.partial(layer_kernel, groups, rank, cap, per_owner),
            out_shape=pltpu.VMEM((toks, width), BF),
            in_specs=[pl.BlockSpec(memory_space=pl.ANY)] * 11,
            out_specs=pl.BlockSpec(memory_space=pltpu.VMEM),
            scratch_shapes=[
                pltpu.VMEM((groups, cap, width), BF),
                pltpu.VMEM((groups, cap, width), BF),
                pltpu.VMEM((slots, width), BF),
                pltpu.VMEM((slots, ranks), BF),
                pltpu.VMEM((slots, ranks), BF),
                pltpu.VMEM((ff // SUB, slots, SUB), BF),
                pltpu.VMEM((slots, ranks), F32),
                pltpu.VMEM((cols, groups, cap, SUB), BF),
                pltpu.VMEM((cols, groups, cap, SUB), BF),
                pltpu.VMEM((ranks, width), BF),
                pltpu.VMEM((STEP_SUBS * SUB, ranks), BF),
                pltpu.VMEM((RING * ring_rows, STEP_SUBS * SUB), BF),
                pltpu.VMEM((groups, 1, toks), jnp.int32),
                pltpu.VMEM((slots, 1), jnp.int32),
                pltpu.VMEM((toks, width), BF),
                pltpu.VMEM((1, toks), jnp.int32),
                pltpu.SemaphoreType.DMA((RING, len(GROUPS))),
                pltpu.SemaphoreType.DMA((2,)),
                pltpu.SemaphoreType.DMA,
                pltpu.SemaphoreType.DMA((cols,)),
                pltpu.SemaphoreType.DMA,
                pltpu.SemaphoreType.DMA,
                pltpu.SemaphoreType.DMA,
                pltpu.SemaphoreType.DMA((cols,)),
                pltpu.SemaphoreType.DMA((2,)),
                pltpu.SemaphoreType.DMA,
                pltpu.SemaphoreType.DMA((groups,)),
            ],
            compiler_params=pltpu.CompilerParams(collective_id=0, has_side_effects=True, vmem_limit_bytes=66_400_000),
            name="lora_layer",
        )(x, adapter_id.reshape(1, toks), w_gate, w_up, w_down, flat(a_gate), flat(a_up), flat(b_gate), flat(b_up), flat(a_down), flat(b_down))

    return jax.shard_map(device_step, mesh=mesh, in_specs=(row_spec, id_spec, P(), P(), P(), owned_spec, owned_spec, owned_spec, owned_spec, owned_spec, owned_spec), out_specs=row_spec, check_vma=False)
```

```python
import functools

import jax
import jax.numpy as jnp
from jax import lax
from jax.experimental import pallas as pl
from jax.experimental.pallas import tpu as pltpu
from jax.sharding import PartitionSpec as P

ALPHA = 32
SUB = 256
STEP_SUBS = 5
RING = 3
GROUPS = ((0, 3), (3, 2))
BF = jnp.bfloat16
F32 = jnp.float32


def nn(a, b):
    return jnp.dot(a, b, preferred_element_type=F32)


def nt(a, b):
    return lax.dot_general(a, b, (((1,), (1,)), ((), ())), preferred_element_type=F32)


def count_ge(v, width, groups):
    total = jnp.zeros(v.shape, jnp.int32)
    for g in range(1, groups):
        total += (v >= g * width).astype(jnp.int32)
    return total


def layer_kernel(groups, rank, cap, per_owner, x_hbm, ids_hbm, wg, wu, wd, ag, au, bg, bu, ad, bd, out_ref,
                 send, recv, rows, low_g, low_u, hid, low_d, ret, got, b_buf, ad_t, big, all_ids, first, x_ref, ids_ref,
                 ring_sem, a_sem, b_sem, wd_sem, out_sem, in_sem, rs_sem, rr_sem, x_sem, id_out, id_in):
    toks, width = x_hbm.shape
    ff = wg.shape[1]
    ranks = per_owner * rank
    slots = groups * cap
    scale = ALPHA / rank
    step = STEP_SUBS * SUB
    n_steps = ff // step
    ring_rows = 2 * width + 3 * ranks
    fold = ff // STEP_SUBS
    cols = width // SUB
    whole = ((wg, 0, width), (wu, width, width), (bg, 2 * width, ranks), (bu, 2 * width + ranks, ranks), (ad, 2 * width + 2 * ranks, ranks))
    me = lax.axis_index("data")
    peers = [lax.rem(me + k, groups) for k in (4, 3, 5, 2, 6, 1, 7) if k < groups]

    def start_ring(c, which):
        slot = lax.rem(c, RING)
        for k, (lo, subs) in enumerate(GROUPS):
            col = pl.multiple_of(c * step + lo * SUB, 128)
            for i in which:
                src, off, n = whole[i]
                at = pl.multiple_of(slot * ring_rows + off, 8)
                pltpu.make_async_copy(src.at[:, pl.ds(col, subs * SUB)], big.at[pl.ds(at, n), pl.ds(lo * SUB, subs * SUB)], ring_sem.at[slot, k]).start()

    def landing(dst, sem):
        return pltpu.make_async_copy(dst, dst, sem)

    def ring_wait(c, k):
        slot = lax.rem(c, RING)
        lo, subs = GROUPS[k]
        landing(big.at[pl.ds(pl.multiple_of(slot * ring_rows, 8), ring_rows), pl.ds(lo * SUB, subs * SUB)], ring_sem.at[slot, k]).wait()

    def wd_at(j):
        return pl.multiple_of(ring_rows * (1 + j // 3) + lax.rem(j, 3) * fold, 8)

    def wd_copy(j, q):
        col = pl.multiple_of(j * SUB, 128)
        return pltpu.make_async_copy(wd.at[pl.ds(q * fold, fold), pl.ds(col, SUB)], big.at[pl.ds(wd_at(j), fold), pl.ds(q * SUB, SUB)], wd_sem.at[j])

    def start_wd(j):
        for q in range(STEP_SUBS):
            wd_copy(j, q).start()

    rest = width - step
    x_copies = [pltpu.make_async_copy(ids_hbm, ids_ref, x_sem.at[0]), pltpu.make_async_copy(x_hbm, x_ref, x_sem.at[1])]
    for cp in x_copies:
        cp.start()
    barrier = pltpu.get_barrier_semaphore()
    for p in peers:
        pl.semaphore_signal(barrier, inc=1, device_id={"data": p}, device_id_type=pl.DeviceIdType.MESH)

    t_base = (RING - 1) * ring_rows
    a_base = t_base + 2 * width
    a_copies = []
    for i, src in enumerate((ag, au)):
        a_copies.append(pltpu.make_async_copy(src.at[:, :step], big.at[pl.ds(a_base + i * ranks, ranks), :], a_sem.at[i]))
        a_copies.append(pltpu.make_async_copy(src.at[:, step:], big.at[pl.ds(a_base + 2 * ranks, ranks), pl.ds(i * rest, rest)], a_sem.at[i]))
    b_copy = pltpu.make_async_copy(bd, b_buf, b_sem)
    for cp in a_copies:
        cp.start()
    for c in range(2):
        start_ring(c, range(len(whole)))
    b_copy.start()

    for cp in x_copies:
        cp.wait()
    id_row = ids_ref[...]
    sub_i = lax.broadcasted_iota(jnp.int32, (toks, toks), 0)
    lane_i = lax.broadcasted_iota(jnp.int32, (toks, toks), 1)
    id_col = jnp.sum(jnp.where(sub_i == lane_i, jnp.broadcast_to(id_row, (toks, toks)), 0), axis=1, keepdims=True)
    own_row = count_ge(id_row, per_owner, groups)
    own_col = count_ge(id_col, per_owner, groups)
    same = own_col == own_row
    arr_col = jnp.sum((same & (lane_i < sub_i)).astype(jnp.int32), axis=1, keepdims=True)
    arr_row = jnp.sum((same & (sub_i < lane_i)).astype(jnp.int32), axis=0, keepdims=True)
    to_slot = (lax.broadcasted_iota(jnp.int32, (slots, toks), 0) == own_row * cap + arr_row).astype(F32).astype(BF)
    send[...] = nn(to_slot, x_ref[...]).reshape(groups, cap, width).astype(BF)

    with jax.named_scope('entry_wait'):
        pl.semaphore_wait(barrier, groups - 1)

    def row_copy(p):
        return pltpu.make_async_remote_copy(src_ref=send.at[p], dst_ref=recv.at[me], send_sem=out_sem, recv_sem=in_sem,
                                            device_id={"data": p}, device_id_type=pl.DeviceIdType.MESH)

    def id_copy(p, at):
        return pltpu.make_async_remote_copy(src_ref=ids_ref, dst_ref=all_ids.at[at], send_sem=id_out, recv_sem=id_in.at[at],
                                            device_id={"data": p}, device_id_type=pl.DeviceIdType.MESH)

    for p in peers:
        id_copy(p, me).start()
    for p in peers:
        row_copy(p).start()
    all_ids[me] = ids_ref[...]
    recv[me] = send[me]
    for i in range(2):
        landing(b_buf, a_sem.at[i]).wait()
    for i in range(2):
        for r in range(0, ranks, 128):
            turned = pl.ds(r, 128)
            big[t_base + i * width:t_base + i * width + step, turned] = big[a_base + i * ranks + r:a_base + i * ranks + r + 128, :].T
            big[t_base + i * width + step:t_base + (i + 1) * width, turned] = big[a_base + 2 * ranks + r:a_base + 2 * ranks + r + 128, i * rest:(i + 1) * rest].T
    start_ring(RING - 1, range(2, len(whole)))
    for p in peers:
        id_copy(p, p).wait_recv()
    every = jnp.concatenate([all_ids[g] for g in range(groups)], axis=0)
    every = every - me * per_owner
    mine = ((every >= 0) & (every < per_owner)).astype(F32)
    before = nn(mine.astype(BF), (sub_i < lane_i).astype(F32).astype(BF))
    slot_i = lax.broadcasted_iota(jnp.int32, (cap, toks), 0).astype(F32)
    value = mine * (every * rank).astype(F32)
    first[...] = jnp.concatenate([jnp.sum(jnp.where(slot_i == before[g:g + 1, :], value[g:g + 1, :], 0.0), axis=1, keepdims=True) for g in range(groups)], axis=0).astype(jnp.int32)

    def own():
        rank_i = lax.broadcasted_iota(jnp.int32, (slots, ranks), 1)
        return (rank_i >= first[...]) & (rank_i < first[...] + rank)

    with jax.named_scope('row_wait'):
        landing(recv.at[:groups - 1], in_sem).wait()

    rows[...] = recv[...].astype(F32).reshape(slots, width).astype(BF)
    lows = [nn(rows[...], big[t_base + i * width:t_base + (i + 1) * width, :ranks]) for i in range(2)]
    low_g[...] = jnp.where(own(), lows[0], 0.0).astype(BF)
    low_u[...] = jnp.where(own(), lows[1], 0.0).astype(BF)
    start_ring(RING - 1, range(2))
    low_d[...] = jnp.zeros_like(low_d)

    def half(base, col, w_off, w_n, b_off, low):
        full = nn(low[...], big[pl.ds(base + b_off, ranks), col])
        return nn(rows[...], big[pl.ds(base + w_off, w_n), col]) + (scale * full).astype(BF).astype(F32)

    def ff_step(c, carry):
        base = pl.multiple_of(lax.rem(c, RING) * ring_rows, 8)
        for k, (lo, subs) in enumerate(GROUPS):
            with jax.named_scope('ring_wait'):
                ring_wait(c, k)
            for s in range(lo, lo + subs):
                col = pl.ds(s * SUB, SUB)
                ad_t[s * SUB:(s + 1) * SUB, :] = big[pl.ds(base + 2 * width + 2 * ranks, ranks), col].T
                g = half(base, col, 0, width, 2 * width, low_g)
                u = half(base, col, width, width, 2 * width + ranks, low_u)
                hid[c * STEP_SUBS + s] = (g * jax.nn.sigmoid(g) * u).astype(BF)
        h = jnp.concatenate([hid[c * STEP_SUBS + s] for s in range(STEP_SUBS)], axis=1)
        low_d[...] += nn(h, ad_t[...])

        @pl.when(c + RING < n_steps)
        def _():
            start_ring(c + RING, range(len(whole)))

        for back in (0, 1):
            @pl.when(c == n_steps - 3 + back)
            def _(back=back):
                for j in range(3 * back, 3 * back + 3):
                    start_wd(j)

        return carry

    lax.fori_loop(0, n_steps, ff_step, 0)

    low_dm = jnp.where(own(), low_d[...], 0.0).astype(BF)
    low_g[...] = low_dm
    b_copy.wait()

    def back_copy(j, n, p):
        return pltpu.make_async_remote_copy(src_ref=ret.at[pl.ds(j, n), p], dst_ref=got.at[pl.ds(j, n), me], send_sem=rs_sem, recv_sem=rr_sem.at[j],
                                            device_id={"data": p}, device_id_type=pl.DeviceIdType.MESH)

    def columns(j, n):
        with jax.named_scope('wd_wait'):
            for k in range(n):
                landing(big.at[pl.ds(wd_at(j + k), fold), :], wd_sem.at[j + k]).wait()
        col = pl.ds(pl.multiple_of(j * SUB, 128), n * SUB)
        full = nn(low_g[...], b_buf[:, col])
        h = jnp.concatenate([hid[s] for s in range(ff // SUB)], axis=1)
        w = jnp.concatenate([jnp.concatenate([big[pl.ds(wd_at(j + k), fold), pl.ds(q * SUB, SUB)] for q in range(STEP_SUBS)], axis=0) for k in range(n)], axis=1)
        done = rows[:, col].astype(F32) + (nn(h, w) + (scale * full).astype(BF).astype(F32))
        for k in range(n):
            ret[j + k] = done[:, k * SUB:(k + 1) * SUB].reshape(groups, cap, SUB).astype(BF)
        for p in peers:
            back_copy(j, n, p).start()
        for k in range(n):
            got[j + k, me] = ret[j + k, me]

    def col_step(j, carry):
        columns(j, 1)
        return carry

    lax.fori_loop(0, cols, col_step, 0)

    to_tok = (lax.broadcasted_iota(jnp.int32, (toks, slots), 1) == own_col * cap + arr_col).astype(F32).astype(BF)
    for j, n in [(j, 1) for j in range(cols)]:
        with jax.named_scope('back_wait'):
            landing(got.at[pl.ds(j, n), :groups - 1], rr_sem.at[j]).wait()
        for k in range(j, j + n):
            block = got[k].astype(F32).reshape(slots, SUB).astype(BF)
            out_ref[:, k * SUB:(k + 1) * SUB] = nn(to_tok, block).astype(BF)
    with jax.named_scope('send_wait'):
        for p in peers:
            id_copy(p, p).wait_send()
        landing(send.at[:groups - 1], out_sem).wait()
        landing(ret.at[:, :groups - 1], rs_sem).wait()


def solution(mesh):
    groups = mesh.shape["data"]
    row_spec = P(("rep", "data"), None)
    id_spec = P(("rep", "data"))
    owned_spec = P("data", None, None)

    def device_step(x, adapter_id, w_gate, w_up, w_down, a_gate, b_gate, a_up, b_up, a_down, b_down):
        toks, width = x.shape
        per_owner, rank, ff = b_gate.shape
        ranks = per_owner * rank
        cap = (3 * toks + groups - 1) // groups
        slots = groups * cap
        cols = width // SUB
        ring_rows = 2 * width + 3 * ranks

        def flat(m):
            return m.reshape(ranks, m.shape[-1])

        return pl.pallas_call(
            functools.partial(layer_kernel, groups, rank, cap, per_owner),
            out_shape=pltpu.VMEM((toks, width), BF),
            in_specs=[pl.BlockSpec(memory_space=pl.ANY)] * 11,
            out_specs=pl.BlockSpec(memory_space=pltpu.VMEM),
            scratch_shapes=[
                pltpu.VMEM((groups, cap, width), BF),
                pltpu.VMEM((groups, cap, width), BF),
                pltpu.VMEM((slots, width), BF),
                pltpu.VMEM((slots, ranks), BF),
                pltpu.VMEM((slots, ranks), BF),
                pltpu.VMEM((ff // SUB, slots, SUB), BF),
                pltpu.VMEM((slots, ranks), F32),
                pltpu.VMEM((cols, groups, cap, SUB), BF),
                pltpu.VMEM((cols, groups, cap, SUB), BF),
                pltpu.VMEM((ranks, width), BF),
                pltpu.VMEM((STEP_SUBS * SUB, ranks), BF),
                pltpu.VMEM((RING * ring_rows, STEP_SUBS * SUB), BF),
                pltpu.VMEM((groups, 1, toks), jnp.int32),
                pltpu.VMEM((slots, 1), jnp.int32),
                pltpu.VMEM((toks, width), BF),
                pltpu.VMEM((1, toks), jnp.int32),
                pltpu.SemaphoreType.DMA((RING, len(GROUPS))),
                pltpu.SemaphoreType.DMA((2,)),
                pltpu.SemaphoreType.DMA,
                pltpu.SemaphoreType.DMA((cols,)),
                pltpu.SemaphoreType.DMA,
                pltpu.SemaphoreType.DMA,
                pltpu.SemaphoreType.DMA,
                pltpu.SemaphoreType.DMA((cols,)),
                pltpu.SemaphoreType.DMA((2,)),
                pltpu.SemaphoreType.DMA,
                pltpu.SemaphoreType.DMA((groups,)),
            ],
            compiler_params=pltpu.CompilerParams(collective_id=0, has_side_effects=True, vmem_limit_bytes=66_400_000),
            name="lora_layer",
        )(x, adapter_id.reshape(1, toks), w_gate, w_up, w_down, flat(a_gate), flat(a_up), flat(b_gate), flat(b_up), flat(a_down), flat(b_down))

    return jax.shard_map(device_step, mesh=mesh, in_specs=(row_spec, id_spec, P(), P(), P(), owned_spec, owned_spec, owned_spec, owned_spec, owned_spec, owned_spec), out_specs=row_spec, check_vma=False)
```

```python
import functools

import jax
import jax.numpy as jnp
from jax import lax
from jax.experimental import pallas as pl
from jax.experimental.pallas import tpu as pltpu
from jax.sharding import PartitionSpec as P

ALPHA = 32
SUB = 256
STEP_SUBS = 5
RING = 3
GROUPS = ((0, 3), (3, 2))
BF = jnp.bfloat16
F32 = jnp.float32


def nn(a, b):
    return jnp.dot(a, b, preferred_element_type=F32)


def nt(a, b):
    return lax.dot_general(a, b, (((1,), (1,)), ((), ())), preferred_element_type=F32)


def count_ge(v, width, groups):
    total = jnp.zeros(v.shape, jnp.int32)
    for g in range(1, groups):
        total += (v >= g * width).astype(jnp.int32)
    return total


def layer_kernel(groups, rank, cap, per_owner, x_hbm, ids_hbm, wg, wu, wd, ag, au, bg, bu, ad, bd, out_ref,
                 send, recv, rows, low_g, low_u, hid, low_d, ret, got, b_buf, ad_t, big, all_ids, first, x_ref, ids_ref,
                 ring_sem, a_sem, b_sem, wd_sem, out_sem, in_sem, rs_sem, rr_sem, x_sem, id_out, id_in):
    toks, width = x_hbm.shape
    ff = wg.shape[1]
    ranks = per_owner * rank
    slots = groups * cap
    scale = ALPHA / rank
    step = STEP_SUBS * SUB
    n_steps = ff // step
    ring_rows = 2 * width + 3 * ranks
    fold = ff // STEP_SUBS
    cols = width // SUB
    whole = ((wg, 0, width), (wu, width, width), (bg, 2 * width, ranks), (bu, 2 * width + ranks, ranks), (ad, 2 * width + 2 * ranks, ranks))
    me = lax.axis_index("data")
    peers = [lax.rem(me + k, groups) for k in (4, 3, 5, 2, 6, 1, 7) if k < groups]

    def start_ring(c, which):
        slot = lax.rem(c, RING)
        for k, (lo, subs) in enumerate(GROUPS):
            col = pl.multiple_of(c * step + lo * SUB, 128)
            for i in which:
                src, off, n = whole[i]
                at = pl.multiple_of(slot * ring_rows + off, 8)
                pltpu.make_async_copy(src.at[:, pl.ds(col, subs * SUB)], big.at[pl.ds(at, n), pl.ds(lo * SUB, subs * SUB)], ring_sem.at[slot, k]).start()

    def landing(dst, sem):
        return pltpu.make_async_copy(dst, dst, sem)

    def ring_wait(c, k):
        slot = lax.rem(c, RING)
        lo, subs = GROUPS[k]
        landing(big.at[pl.ds(pl.multiple_of(slot * ring_rows, 8), ring_rows), pl.ds(lo * SUB, subs * SUB)], ring_sem.at[slot, k]).wait()

    def wd_at(j):
        return pl.multiple_of(ring_rows * (1 + j // 3) + lax.rem(j, 3) * fold, 8)

    def wd_copy(j, q):
        col = pl.multiple_of(j * SUB, 128)
        return pltpu.make_async_copy(wd.at[pl.ds(q * fold, fold), pl.ds(col, SUB)], big.at[pl.ds(wd_at(j), fold), pl.ds(q * SUB, SUB)], wd_sem.at[j])

    def start_wd(j):
        for q in range(STEP_SUBS):
            wd_copy(j, q).start()

    rest = width - step
    x_copies = [pltpu.make_async_copy(ids_hbm, ids_ref, x_sem.at[0]), pltpu.make_async_copy(x_hbm, x_ref, x_sem.at[1])]
    for cp in x_copies:
        cp.start()
    barrier = pltpu.get_barrier_semaphore()
    for p in peers:
        pl.semaphore_signal(barrier, inc=1, device_id={"data": p}, device_id_type=pl.DeviceIdType.MESH)

    t_base = (RING - 1) * ring_rows
    a_base = t_base + 2 * width
    a_copies = []
    for i, src in enumerate((ag, au)):
        a_copies.append(pltpu.make_async_copy(src.at[:, :step], big.at[pl.ds(a_base + i * ranks, ranks), :], a_sem.at[i]))
        a_copies.append(pltpu.make_async_copy(src.at[:, step:], big.at[pl.ds(a_base + 2 * ranks, ranks), pl.ds(i * rest, rest)], a_sem.at[i]))
    b_copy = pltpu.make_async_copy(bd, b_buf, b_sem)
    for cp in a_copies:
        cp.start()
    for c in range(2):
        start_ring(c, range(len(whole)))

    for cp in x_copies:
        cp.wait()
    id_row = ids_ref[...]
    sub_i = lax.broadcasted_iota(jnp.int32, (toks, toks), 0)
    lane_i = lax.broadcasted_iota(jnp.int32, (toks, toks), 1)
    id_col = jnp.sum(jnp.where(sub_i == lane_i, jnp.broadcast_to(id_row, (toks, toks)), 0), axis=1, keepdims=True)
    own_row = count_ge(id_row, per_owner, groups)
    own_col = count_ge(id_col, per_owner, groups)
    same = own_col == own_row
    arr_col = jnp.sum((same & (lane_i < sub_i)).astype(jnp.int32), axis=1, keepdims=True)
    arr_row = jnp.sum((same & (sub_i < lane_i)).astype(jnp.int32), axis=0, keepdims=True)
    to_slot = (lax.broadcasted_iota(jnp.int32, (slots, toks), 0) == own_row * cap + arr_row).astype(F32).astype(BF)
    send[...] = nn(to_slot, x_ref[...]).reshape(groups, cap, width).astype(BF)

    with jax.named_scope('entry_wait'):
        pl.semaphore_wait(barrier, groups - 1)

    def row_copy(p):
        return pltpu.make_async_remote_copy(src_ref=send.at[p], dst_ref=recv.at[me], send_sem=out_sem, recv_sem=in_sem,
                                            device_id={"data": p}, device_id_type=pl.DeviceIdType.MESH)

    def id_copy(p, at):
        return pltpu.make_async_remote_copy(src_ref=ids_ref, dst_ref=all_ids.at[at], send_sem=id_out, recv_sem=id_in.at[at],
                                            device_id={"data": p}, device_id_type=pl.DeviceIdType.MESH)

    for p in peers:
        id_copy(p, me).start()
    for p in peers:
        row_copy(p).start()
    all_ids[me] = ids_ref[...]
    recv[me] = send[me]
    for i in range(2):
        landing(b_buf, a_sem.at[i]).wait()
    for i in range(2):
        for r in range(0, ranks, 128):
            turned = pl.ds(r, 128)
            big[t_base + i * width:t_base + i * width + step, turned] = big[a_base + i * ranks + r:a_base + i * ranks + r + 128, :].T
            big[t_base + i * width + step:t_base + (i + 1) * width, turned] = big[a_base + 2 * ranks + r:a_base + 2 * ranks + r + 128, i * rest:(i + 1) * rest].T
    start_ring(RING - 1, range(2, len(whole)))
    for p in peers:
        id_copy(p, p).wait_recv()
    every = jnp.concatenate([all_ids[g] for g in range(groups)], axis=0)
    every = every - me * per_owner
    mine = ((every >= 0) & (every < per_owner)).astype(F32)
    before = nn(mine.astype(BF), (sub_i < lane_i).astype(F32).astype(BF))
    slot_i = lax.broadcasted_iota(jnp.int32, (cap, toks), 0).astype(F32)
    value = mine * (every * rank).astype(F32)
    first[...] = jnp.concatenate([jnp.sum(jnp.where(slot_i == before[g:g + 1, :], value[g:g + 1, :], 0.0), axis=1, keepdims=True) for g in range(groups)], axis=0).astype(jnp.int32)

    def own():
        rank_i = lax.broadcasted_iota(jnp.int32, (slots, ranks), 1)
        return (rank_i >= first[...]) & (rank_i < first[...] + rank)

    with jax.named_scope('row_wait'):
        landing(recv.at[:groups - 1], in_sem).wait()

    rows[...] = recv[...].astype(F32).reshape(slots, width).astype(BF)
    lows = [nn(rows[...], big[t_base + i * width:t_base + (i + 1) * width, :ranks]) for i in range(2)]
    low_g[...] = jnp.where(own(), lows[0], 0.0).astype(BF)
    low_u[...] = jnp.where(own(), lows[1], 0.0).astype(BF)
    start_ring(RING - 1, range(2))
    low_d[...] = jnp.zeros_like(low_d)

    def half(base, col, w_off, w_n, b_off, low):
        full = nn(low[...], big[pl.ds(base + b_off, ranks), col])
        return nn(rows[...], big[pl.ds(base + w_off, w_n), col]) + (scale * full).astype(BF).astype(F32)

    def ff_step(c, carry):
        base = pl.multiple_of(lax.rem(c, RING) * ring_rows, 8)
        for k, (lo, subs) in enumerate(GROUPS):
            with jax.named_scope('ring_wait'):
                ring_wait(c, k)
            for s in range(lo, lo + subs):
                col = pl.ds(s * SUB, SUB)
                ad_t[s * SUB:(s + 1) * SUB, :] = big[pl.ds(base + 2 * width + 2 * ranks, ranks), col].T
                g = half(base, col, 0, width, 2 * width, low_g)
                u = half(base, col, width, width, 2 * width + ranks, low_u)
                hid[c * STEP_SUBS + s] = (g * jax.nn.sigmoid(g) * u).astype(BF)
        h = jnp.concatenate([hid[c * STEP_SUBS + s] for s in range(STEP_SUBS)], axis=1)
        low_d[...] += nn(h, ad_t[...])

        @pl.when(c + RING < n_steps)
        def _():
            start_ring(c + RING, range(len(whole)))

        for back in (0, 1):
            @pl.when(c == n_steps - 3 + back)
            def _(back=back):
                if back == 0:
                    b_copy.start()
                for j in range(3 * back, 3 * back + 3):
                    start_wd(j)

        return carry

    lax.fori_loop(0, n_steps, ff_step, 0)

    low_dm = jnp.where(own(), low_d[...], 0.0).astype(BF)
    low_g[...] = low_dm
    b_copy.wait()

    def back_copy(j, n, p):
        return pltpu.make_async_remote_copy(src_ref=ret.at[pl.ds(j, n), p], dst_ref=got.at[pl.ds(j, n), me], send_sem=rs_sem, recv_sem=rr_sem.at[j],
                                            device_id={"data": p}, device_id_type=pl.DeviceIdType.MESH)

    def columns(j, n):
        with jax.named_scope('wd_wait'):
            for k in range(n):
                landing(big.at[pl.ds(wd_at(j + k), fold), :], wd_sem.at[j + k]).wait()
        col = pl.ds(pl.multiple_of(j * SUB, 128), n * SUB)
        full = nn(low_g[...], b_buf[:, col])
        h = jnp.concatenate([hid[s] for s in range(ff // SUB)], axis=1)
        w = jnp.concatenate([jnp.concatenate([big[pl.ds(wd_at(j + k), fold), pl.ds(q * SUB, SUB)] for q in range(STEP_SUBS)], axis=0) for k in range(n)], axis=1)
        done = rows[:, col].astype(F32) + (nn(h, w) + (scale * full).astype(BF).astype(F32))
        for k in range(n):
            ret[j + k] = done[:, k * SUB:(k + 1) * SUB].reshape(groups, cap, SUB).astype(BF)
        for p in peers:
            back_copy(j, n, p).start()
        for k in range(n):
            got[j + k, me] = ret[j + k, me]

    def col_step(j, carry):
        columns(j, 1)
        return carry

    lax.fori_loop(0, cols, col_step, 0)

    to_tok = (lax.broadcasted_iota(jnp.int32, (toks, slots), 1) == own_col * cap + arr_col).astype(F32).astype(BF)
    for j, n in [(j, 1) for j in range(cols)]:
        with jax.named_scope('back_wait'):
            landing(got.at[pl.ds(j, n), :groups - 1], rr_sem.at[j]).wait()
        for k in range(j, j + n):
            block = got[k].astype(F32).reshape(slots, SUB).astype(BF)
            out_ref[:, k * SUB:(k + 1) * SUB] = nn(to_tok, block).astype(BF)
    with jax.named_scope('send_wait'):
        for p in peers:
            id_copy(p, p).wait_send()
        landing(send.at[:groups - 1], out_sem).wait()
        landing(ret.at[:, :groups - 1], rs_sem).wait()


def solution(mesh):
    groups = mesh.shape["data"]
    row_spec = P(("rep", "data"), None)
    id_spec = P(("rep", "data"))
    owned_spec = P("data", None, None)

    def device_step(x, adapter_id, w_gate, w_up, w_down, a_gate, b_gate, a_up, b_up, a_down, b_down):
        toks, width = x.shape
        per_owner, rank, ff = b_gate.shape
        ranks = per_owner * rank
        cap = (3 * toks + groups - 1) // groups
        slots = groups * cap
        cols = width // SUB
        ring_rows = 2 * width + 3 * ranks

        def flat(m):
            return m.reshape(ranks, m.shape[-1])

        return pl.pallas_call(
            functools.partial(layer_kernel, groups, rank, cap, per_owner),
            out_shape=pltpu.VMEM((toks, width), BF),
            in_specs=[pl.BlockSpec(memory_space=pl.ANY)] * 11,
            out_specs=pl.BlockSpec(memory_space=pltpu.VMEM),
            scratch_shapes=[
                pltpu.VMEM((groups, cap, width), BF),
                pltpu.VMEM((groups, cap, width), BF),
                pltpu.VMEM((slots, width), BF),
                pltpu.VMEM((slots, ranks), BF),
                pltpu.VMEM((slots, ranks), BF),
                pltpu.VMEM((ff // SUB, slots, SUB), BF),
                pltpu.VMEM((slots, ranks), F32),
                pltpu.VMEM((cols, groups, cap, SUB), BF),
                pltpu.VMEM((cols, groups, cap, SUB), BF),
                pltpu.VMEM((ranks, width), BF),
                pltpu.VMEM((STEP_SUBS * SUB, ranks), BF),
                pltpu.VMEM((RING * ring_rows, STEP_SUBS * SUB), BF),
                pltpu.VMEM((groups, 1, toks), jnp.int32),
                pltpu.VMEM((slots, 1), jnp.int32),
                pltpu.VMEM((toks, width), BF),
                pltpu.VMEM((1, toks), jnp.int32),
                pltpu.SemaphoreType.DMA((RING, len(GROUPS))),
                pltpu.SemaphoreType.DMA((2,)),
                pltpu.SemaphoreType.DMA,
                pltpu.SemaphoreType.DMA((cols,)),
                pltpu.SemaphoreType.DMA,
                pltpu.SemaphoreType.DMA,
                pltpu.SemaphoreType.DMA,
                pltpu.SemaphoreType.DMA((cols,)),
                pltpu.SemaphoreType.DMA((2,)),
                pltpu.SemaphoreType.DMA,
                pltpu.SemaphoreType.DMA((groups,)),
            ],
            compiler_params=pltpu.CompilerParams(collective_id=0, has_side_effects=True, vmem_limit_bytes=66_400_000),
            name="lora_layer",
        )(x, adapter_id.reshape(1, toks), w_gate, w_up, w_down, flat(a_gate), flat(a_up), flat(b_gate), flat(b_up), flat(a_down), flat(b_down))

    return jax.shard_map(device_step, mesh=mesh, in_specs=(row_spec, id_spec, P(), P(), P(), owned_spec, owned_spec, owned_spec, owned_spec, owned_spec, owned_spec), out_specs=row_spec, check_vma=False)
```
